256 devices in a mesh: region: 32 (over x, z), member: 8 (over y, core).
Axes of the slice: x: 4, y: 4, z: 8, core: 2. Of those that a mesh axis runs over, the one named last changes fastest.
Arguments:
- ensemble: bfloat16 [80, 524288], P('member', 'region'), may hold values from -6 to 6
- obs_value: float32 [8192, 128], P(('region', 'member')), may hold values from -8 to 8
- obs_var: float32 [8192, 128], P(('region', 'member')), may hold values from 0.1 to 1
- obs_point: int32 [8192, 128], P(('region', 'member')), may hold values from 0 to 16383
- owned_blocks: int32 [4096], P('region'), may hold values from 0 to 4095, each once
- infl_mean: float32 [4096], replicated, may hold values from 0.6 to 1.6
- infl_var: float32 [4096], replicated, may hold values from 0.0001 to 0.1
Outputs:
- inflated: bfloat16 [80, 524288], P('member', 'region')
- infl_post: float32 [4096], P(('region', 'member'))
The draws below stay inside these ranges and needn't reach their ends.
Inputs may be any that keep to these rules, and one draw needn't show every extreme that they name: `obs_point`: index among the 16384 points of the observation's region; the observation belongs to the block of that point's slot. `owned_blocks`: every block id appears exactly once.
All inputs are finite; a program needn't handle non-finite values.
Results may differ from the reference program's by a relative error of at most 0.001.
Values sent between devices are 32-bit elements; how exact they have to be, the bound alone decides.
A program may use at most 64 MiB of HBM per device.

```python
import math
import jax
import jax.numpy as jnp
from jax import lax

PTS_DEV = 16384
OBS_DEV = 4096
MEMBERS = 80
PTS = 524288
BLOCKS = 4096
SPAN = 128
OBS_ROWS = 8192
N_MEMBER = 8


def with_ends(values, rng, low, top_value):
    shape = values.shape
    index_at = [jax.random.randint(jax.random.fold_in(rng, axis), (), 0, shape[axis]) for axis in range(len(shape))]
    values = values.at[tuple(index_at)].set(low)
    longest = shape.index(max(shape))
    index_at[longest] = (index_at[longest] + 1) % shape[longest]
    return values.at[tuple(index_at)].set(top_value)


def block_scale(rng, shape, shards, least, largest):
    def one(position, shards_of):
        heights = jax.random.uniform(jax.random.fold_in(jax.random.fold_in(rng, 6), position), (shards_of,), jnp.float32, least / len(shards), largest / len(shards))
        return jnp.repeat(jnp.exp(heights), shape[position] // shards_of).reshape((-1,) + (1,) * (len(shape) - position - 1))

    loudness = one(*shards[0])
    for cut in shards[1:]:
        loudness = loudness * one(*cut)
    return loudness


def scatter_about(rng, extent, width, reach, shards=(), kind=jnp.bfloat16):
    gain = block_scale(rng, extent, shards, -0.22, 0.18) if shards else 1.0
    result = jax.random.normal(rng, extent, jnp.float32) * width * gain
    return jnp.minimum(jnp.maximum(result, -reach), reach).astype(kind)


def setup_inputs(seed: int = 0) -> dict:
    arg_keys = jax.random.split(jax.random.key(seed), 8)
    return {
        "ensemble": scatter_about(arg_keys[0], (MEMBERS, PTS), 1.0, 6.0, ((0, 8), (1, 32))),
        "obs_value": scatter_about(arg_keys[1], (OBS_ROWS, 128), 1.3, 8.0, ((0, 256),), jnp.float32),
        "obs_var": jnp.clip(jnp.exp(math.log(1.0) - 2.3025851 * jax.random.uniform(arg_keys[2], (OBS_ROWS, 128), jnp.float32) ** block_scale(arg_keys[2], (OBS_ROWS, 128), ((0, 256),), -0.2, 0.2)), 0.1, 1.0),
        "obs_point": with_ends(jax.random.randint(arg_keys[3], (OBS_ROWS, 128), 0, PTS_DEV), jax.random.fold_in(arg_keys[3], 1), 0, PTS_DEV - 1).astype(jnp.int32),
        "owned_blocks": jax.random.permutation(arg_keys[4], BLOCKS).astype(jnp.int32),
        "infl_mean": jnp.clip(jax.random.uniform(arg_keys[5], (BLOCKS,), jnp.float32, 0.6, 1.6), 0.6, 1.6),
        "infl_var": jnp.clip(jnp.exp(jax.random.uniform(arg_keys[6], (BLOCKS,), jnp.float32, math.log(0.0001), math.log(0.1))), 0.0001, 0.1),
    }


def posterior(sums, prior_mean, prior_var):
    innov_sum = sums[0]
    spread_sum = sums[1]
    error_sum = sums[2]
    spread_spread = sums[3]
    spread_error = sums[4]
    error_error = sums[5]
    weight_var = 2.0 * prior_mean * prior_mean * (1.0 + spread_spread) + 4.0 * prior_mean * spread_error + 2.0 * error_error
    value = (prior_mean * weight_var + prior_var * spread_sum * (innov_sum - error_sum)) / (weight_var + prior_var * spread_sum * spread_sum)
    return jnp.maximum(value, 1.0)

def reference(ensemble, obs_value, obs_var, obs_point, owned_blocks, infl_mean, infl_var):
    wide = ensemble.astype(jnp.float32)
    point_total = lax.optimization_barrier(jnp.sum(wide, 0))
    point_square = lax.optimization_barrier(jnp.sum(wide * wide, 0))
    point_mean = point_total / MEMBERS
    row_region = jnp.arange(OBS_ROWS, dtype=jnp.int32) // (OBS_DEV // 128 * N_MEMBER)
    global_point = (row_region[:, None] * PTS_DEV + obs_point).reshape(-1).astype(jnp.int32)
    at_mean = point_mean[global_point]
    at_square = point_square[global_point]
    spread = (at_square - MEMBERS * at_mean * at_mean) / (MEMBERS - 1)
    innovation = obs_value.reshape(-1) - at_mean
    errors = obs_var.reshape(-1)
    obs_blk = owned_blocks[(global_point // SPAN).astype(jnp.int32)].astype(jnp.int32)
    columns = jnp.stack([innovation * innovation, spread, errors, spread * spread, spread * errors, errors * errors], 1)
    sums = jax.ops.segment_sum(columns, obs_blk, num_segments=BLOCKS)
    infl_post = posterior(sums.T, infl_mean, infl_var)
    point_lambda = jnp.repeat(infl_post[owned_blocks], SPAN)
    inflated = (point_mean + jnp.sqrt(point_lambda) * (wide - point_mean)).astype(jnp.bfloat16)
    return (inflated, infl_post)
```

```python
import functools

import jax
import jax.numpy as jnp
from jax import lax
from jax.experimental import pallas as pl
from jax.experimental.pallas import tpu as pltpu
from jax.sharding import PartitionSpec as P

MESH = pl.DeviceIdType.MESH
F32 = jnp.float32
BF16 = jnp.bfloat16
OWN = 16
LANES = 128
PIECE = 5 * OWN + 8


def parts_of(x):
    first = x.astype(BF16).astype(F32)
    rest = x - first
    second = rest.astype(BF16).astype(F32)
    return first, second, (rest - second).astype(BF16).astype(F32)


def point_sums(ens_v, sums):
    @pl.loop(0, 16)
    def _(j):
        x = ens_v[:, pl.ds(pl.multiple_of(j * 1024, 1024), 1024)].astype(F32)
        total = jnp.sum(x, axis=0, keepdims=True)
        square = jnp.sum(x * x, axis=0, keepdims=True)
        piece = sums.at[(j // 2) % 2, j // 4]
        for i in range(8):
            row = 8 * (j % 2) + i
            piece[pl.ds(row, 1), :] = total[:, i * LANES : (i + 1) * LANES]
            piece[pl.ds(OWN + row, 1), :] = square[:, i * LANES : (i + 1) * LANES]


def histograms(val_v, var_v, pnt_v, acc, acc_q, sums):
    rows = 4
    across = (((1,), (1,)), ((), ()))
    acc[...] = jnp.zeros_like(acc)
    acc_q[...] = jnp.zeros_like(acc_q)

    @pl.loop(0, 32 // rows)
    def _(step):
        left, right, square = [], [], []
        for i in range(rows):
            at = pl.ds(step * rows + i, 1)
            point, value, var = pnt_v[at, :], val_v[at, :], var_v[at, :]
            index = lax.broadcasted_iota(jnp.int32, (LANES, LANES), 0)
            in_slot = index == point // LANES
            in_lane = index == point % LANES
            v1, v2, _ = parts_of(value)
            e1, e2, _ = parts_of(var)
            zero = jnp.zeros((LANES, LANES), F32)
            left.append(
                jnp.concatenate(
                    [
                        jnp.where(in_slot, jnp.broadcast_to(w, (LANES, LANES)), zero).astype(BF16)
                        for w in (jnp.ones_like(v1), v1, v2, e1, e2)
                    ],
                    axis=0,
                )
            )
            right.append(jnp.where(in_lane, 1.0, zero).astype(BF16))
            none = jnp.zeros_like(v1)
            square.append(
                jnp.concatenate(
                    [*parts_of(value * value), *parts_of(var * var), none, none], axis=0
                ).astype(BF16)
            )
        left = jnp.concatenate(left, axis=1)
        right = jnp.concatenate(right, axis=1)
        square = jnp.concatenate(square, axis=1)
        acc[...] += lax.dot_general(left, right, across, preferred_element_type=F32)
        acc_q[...] += lax.dot_general(square, left[:LANES], across, preferred_element_type=F32)

    for g in range(8):
        at = slice(g * OWN, (g + 1) * OWN)
        part = [acc[k * LANES + g * OWN : k * LANES + (g + 1) * OWN, :] for k in range(5)]
        piece = sums.at[g % 2, g // 2]
        piece[2 * OWN : 3 * OWN, :] = part[0]
        piece[3 * OWN : 4 * OWN, :] = part[1] + part[2]
        piece[4 * OWN : 5 * OWN, :] = part[3] + part[4]
        piece[5 * OWN :, :] = acc_q[...]


def kernel(
    ens, val, var, pnt, own, mean_tab, var_tab,
    out, post,
    ens_v, val_v, var_v, pnt_v, own_v, mean_v, ivar_v, out_v,
    acc, acc_q, sums, from_core, to_chip, from_chip, means, my_lam, lams, scale, to_region, from_region,
    load_sem, store_sem, core_send, core_recv, chip_send, chip_recv,
    mean_send, mean_recv, lam_send, lam_recv, reg_send, reg_recv,
):
    region, member = lax.axis_index("region"), lax.axis_index("member")
    regions, members = 32, 8
    y, core = member // 2, member % 2

    barrier = pltpu.get_barrier_semaphore()
    for d in range(1, regions):
        pl.semaphore_signal(
            barrier, inc=1, device_id={"region": (region + d) % regions}, device_id_type=MESH
        )
    for d in range(1, members):
        pl.semaphore_signal(
            barrier, inc=1, device_id={"member": (member + d) % members}, device_id_type=MESH
        )

    loads = [
        pltpu.make_async_copy(a, b, load_sem.at[i])
        for i, (a, b) in enumerate(
            (
                (ens, ens_v),
                (pnt, pnt_v),
                (val, val_v),
                (var, var_v),
                (own, own_v),
                (mean_tab, mean_v),
                (var_tab, ivar_v),
            )
        )
    ]
    for load in loads:
        load.start()
    for load in loads:
        load.wait()

    point_sums(ens_v, sums)
    histograms(val_v, var_v, pnt_v, acc, acc_q, sums)

    sub = lax.broadcasted_iota(jnp.int32, (LANES, LANES), 0)
    lane = lax.broadcasted_iota(jnp.int32, (LANES, LANES), 1)
    eye = sub == lane
    ids = own_v[...]
    ids_col = jnp.sum(jnp.where(eye, ids.astype(F32), 0.0), axis=1, keepdims=True).astype(jnp.int32)
    in_row = (
        lax.broadcasted_iota(jnp.int32, (LANES, 32), 1) == ids_col // LANES
    ).astype(F32)

    def looked_up(table):
        picked = jnp.dot(
            in_row, table[...], precision=lax.Precision.HIGHEST, preferred_element_type=F32
        )
        col = jnp.sum(jnp.where(lane == ids_col % LANES, picked, 0.0), axis=1, keepdims=True)
        return jnp.sum(jnp.where(eye, col, 0.0), axis=0, keepdims=True)

    prior_mean, prior_var = looked_up(mean_v), looked_up(ivar_v)

    pl.semaphore_wait(barrier, regions - 1 + members - 1)

    other = member + 1 - 2 * core
    order = (2, 1, 3, 0)
    core_copies = {}
    for d in order:
        at = (y + d) % 4
        core_copies[d] = pltpu.make_async_remote_copy(
            src_ref=sums.at[1 - core, at],
            dst_ref=from_core.at[d],
            send_sem=core_send.at[d],
            recv_sem=core_recv.at[d],
            device_id={"member": other},
            device_id_type=MESH,
        )
        core_copies[d].start()
    chip_copies = {}
    for d in order:
        core_copies[d].wait_recv()
        to_chip[d] = sums[core, (y + d) % 4] + from_core[d]
        if d:
            chip_copies[d] = pltpu.make_async_remote_copy(
                src_ref=to_chip.at[d],
                dst_ref=from_chip.at[d - 1],
                send_sem=chip_send.at[d - 1],
                recv_sem=chip_recv.at[d - 1],
                device_id={"member": ((y + d) % 4) * 2 + core},
                device_id_type=MESH,
            )
            chip_copies[d].start()
    for d in (1, 3, 2):
        chip_copies[d].wait_recv()

    def summed(k, size=OWN):
        at = slice(k * OWN, k * OWN + size)
        return (to_chip[0, at, :] + from_chip[0, at, :]) + (
            from_chip[1, at, :] + from_chip[2, at, :]
        )

    mean = summed(0) / 80.0
    my_rows = pl.ds(pl.multiple_of(member * OWN, OWN), OWN)
    means[my_rows, :] = mean
    mean_copies = []
    for d in (4, 3, 5, 2, 6, 1, 7):
        mean_copies.append(
            pltpu.make_async_remote_copy(
                src_ref=means.at[my_rows],
                dst_ref=means.at[my_rows],
                send_sem=mean_send.at[d - 1],
                recv_sem=mean_recv.at[d - 1],
                device_id={"member": (member + d) % members},
                device_id_type=MESH,
            )
        )
        mean_copies[-1].start()

    spread = (summed(1) - 80.0 * mean * mean) / 79.0
    count, value, error, squares = summed(2), summed(3), summed(4), summed(5, 8)
    mine = (
        lax.broadcasted_iota(jnp.int32, (OWN, LANES), 1)
        == lax.broadcasted_iota(jnp.int32, (OWN, LANES), 0) + member * OWN
    )

    def per_slot(x):
        col = jnp.sum(x, axis=1, keepdims=True)
        return jnp.sum(jnp.where(mine, col, 0.0), axis=0, keepdims=True)

    innov_sum = jnp.sum(squares[0:3], axis=0, keepdims=True) + per_slot(
        mean * (count * mean - 2.0 * value)
    )
    error_error = jnp.sum(squares[3:6], axis=0, keepdims=True)
    count_spread = count * spread
    spread_sum = per_slot(count_spread)
    spread_spread = per_slot(count_spread * spread)
    spread_error = per_slot(spread * error)
    error_sum = per_slot(error)
    weight_var = (
        2.0 * prior_mean * prior_mean * (1.0 + spread_spread)
        + 4.0 * prior_mean * spread_error
        + 2.0 * error_error
    )
    lam = jnp.maximum(
        (prior_mean * weight_var + prior_var * spread_sum * (innov_sum - error_sum))
        / (weight_var + prior_var * spread_sum * spread_sum),
        1.0,
    )
    lane_row = lax.broadcasted_iota(jnp.int32, (1, LANES), 1)
    my_lam[...] = jnp.where(lane_row // OWN == member, lam, 0.0)
    lam_copies = []
    for d in (4, 3, 5, 2, 6, 1, 7):
        lam_copies.append(
            pltpu.make_async_remote_copy(
                src_ref=my_lam,
                dst_ref=lams.at[d - 1],
                send_sem=lam_send.at[d - 1],
                recv_sem=lam_recv.at[d - 1],
                device_id={"member": (member + d) % members},
                device_id_type=MESH,
            )
        )
        lam_copies[-1].start()
    for copy in lam_copies:
        copy.wait_recv()
    lam_row = my_lam[...]
    for d in range(members - 1):
        lam_row = lam_row + lams[d]
    lam_col = jnp.sum(jnp.where(eye, lam_row, 0.0), axis=1, keepdims=True)

    for g in range(4):
        block = (g * 8 + lane // OWN) * LANES + member * OWN + lane % OWN
        to_region[g] = jnp.sum(jnp.where(ids_col == block, lam_col, 0.0), axis=0, keepdims=True)
    reg_copies = []
    for d in range(1, regions):
        dest = (region + d) % regions
        reg_copies.append(
            pltpu.make_async_remote_copy(
                src_ref=to_region.at[dest // 8],
                dst_ref=from_region.at[d - 1],
                send_sem=reg_send.at[d - 1],
                recv_sem=reg_recv.at[d - 1],
                device_id={"region": dest},
                device_id_type=MESH,
            )
        )
        reg_copies[-1].start()

    for copy in mean_copies:
        copy.wait_recv()
    scale[...] = jnp.broadcast_to(jnp.sqrt(lam_col), (LANES, LANES))

    @pl.loop(0, 16)
    def _(j):
        for i in range(8):
            at = pl.ds(pl.multiple_of(j * 1024 + i * LANES, LANES), LANES)
            row = pl.ds(j * 8 + i, 1)
            m = means[row, :]
            x = ens_v[:, at].astype(F32)
            out_v[:, at] = (m + scale[row, :] * (x - m)).astype(BF16)

    store = pltpu.make_async_copy(out_v, out, store_sem)
    store.start()

    for copy in reg_copies:
        copy.wait_recv()
    post_row = to_region[region // 8]
    for d in range(regions - 1):
        post_row = post_row + from_region[d]
    turned = pltpu.roll(
        jnp.broadcast_to(post_row, (8, LANES)), (8 - region % 8) * OWN % LANES, 1
    )
    post[...] = turned[0:1, :OWN]

    store.wait()
    for copy in (
        *core_copies.values(), *chip_copies.values(), *mean_copies, *lam_copies, *reg_copies
    ):
        copy.wait_send()


def body(ensemble, obs_value, obs_var, obs_point, owned_blocks, infl_mean, infl_var):
    anywhere = pl.BlockSpec(memory_space=pl.ANY)
    vmem = pl.BlockSpec(memory_space=pltpu.VMEM)
    dma = pltpu.SemaphoreType.DMA
    inflated, post = pl.pallas_call(
        kernel,
        out_shape=(
            jax.ShapeDtypeStruct(ensemble.shape, BF16),
            jax.ShapeDtypeStruct((1, OWN), F32),
        ),
        in_specs=[anywhere] * 7,
        out_specs=(anywhere, vmem),
        scratch_shapes=[
            pltpu.VMEM((10, 16384), BF16),
            pltpu.VMEM((32, LANES), F32),
            pltpu.VMEM((32, LANES), F32),
            pltpu.VMEM((32, LANES), jnp.int32),
            pltpu.VMEM((1, LANES), jnp.int32),
            pltpu.VMEM((32, LANES), F32),
            pltpu.VMEM((32, LANES), F32),
            pltpu.VMEM((10, 16384), BF16),
            pltpu.VMEM((5 * LANES, LANES), F32),
            pltpu.VMEM((8, LANES), F32),
            pltpu.VMEM((2, 4, PIECE, LANES), F32),
            pltpu.VMEM((4, PIECE, LANES), F32),
            pltpu.VMEM((4, PIECE, LANES), F32),
            pltpu.VMEM((3, PIECE, LANES), F32),
            pltpu.VMEM((LANES, LANES), F32),
            pltpu.VMEM((1, LANES), F32),
            pltpu.VMEM((7, 1, LANES), F32),
            pltpu.VMEM((LANES, LANES), F32),
            pltpu.VMEM((4, 1, LANES), F32),
            pltpu.VMEM((31, 1, LANES), F32),
            dma((7,)),
            dma,
            dma((4,)),
            dma((4,)),
            dma((3,)),
            dma((3,)),
            dma((7,)),
            dma((7,)),
            dma((7,)),
            dma((7,)),
            dma((31,)),
            dma((31,)),
        ],
        compiler_params=pltpu.CompilerParams(collective_id=0, has_side_effects=True),
    )(
        ensemble,
        obs_value,
        obs_var,
        obs_point,
        owned_blocks.reshape(1, -1),
        infl_mean.reshape(32, LANES),
        infl_var.reshape(32, LANES),
    )
    return inflated, post.reshape(-1)


def solution(mesh):
    placed = (
        P("member", "region"),
        P(("region", "member"), None),
        P(("region", "member"), None),
        P(("region", "member"), None),
        P("region"),
        P(),
        P(),
    )
    return jax.shard_map(
        body,
        mesh=mesh,
        in_specs=placed,
        out_specs=(P("member", "region"), P(("region", "member"))),
        check_vma=False,
    )
```

```python
import jax
import jax.numpy as jnp
from jax import lax
from jax.experimental import pallas as pl
from jax.experimental.pallas import tpu as pltpu
from jax.sharding import PartitionSpec as P

MESH = pl.DeviceIdType.MESH
F32 = jnp.float32
BF16 = jnp.bfloat16
I32 = jnp.int32
OWN = 16
LANES = 128
HALF = 64
PIECE = 5 * OWN + 8
STEP = 8


def parts_of(x, count):
    parts = []
    for _ in range(count):
        parts.append(x.astype(BF16))
        x = x - parts[-1].astype(F32)
    return [p.astype(F32) for p in parts]


def point_sums(ens_v, sums):
    @pl.loop(0, 16)
    def _(j):
        x = ens_v[:, pl.ds(pl.multiple_of(j * 1024, 1024), 1024)].astype(F32)
        total = jnp.sum(x, axis=0, keepdims=True)
        square = jnp.sum(x * x, axis=0, keepdims=True)
        for i in range(8):
            row = 4 * (j % 4) + i // 2
            piece = sums.at[i % 2, j // 4]
            piece[pl.ds(row, 1), :] = total[:, i * LANES : (i + 1) * LANES]
            piece[pl.ds(OWN + row, 1), :] = square[:, i * LANES : (i + 1) * LANES]


def tall(row, rows):
    same = jnp.broadcast_to(row, (16, LANES)).astype(BF16)
    return jnp.concatenate([same] * (rows // 16), axis=0)


def histograms(val_v, var_v, pnt_v, acc, acc_q, sums):
    across = (((1,), (1,)), ((), ()))
    index = lax.broadcasted_iota(I32, (256, LANES), 0).astype(F32).astype(BF16)
    none, one = jnp.zeros((256, LANES), BF16), jnp.ones((256, LANES), BF16)
    acc[...] = jnp.zeros_like(acc)
    acc_q[...] = jnp.zeros_like(acc_q)

    @pl.loop(0, 32 // STEP)
    def _(step):
        left, right, square = [], [], []
        for i in range(STEP):
            at = pl.ds(step * STEP + i, 1)
            point, value, var = pnt_v[at, :], val_v[at, :], var_v[at, :]
            in_high = index[:HALF] == tall((point >> 8).astype(F32), HALF)
            in_low = index == tall((point & 255).astype(F32), 256)
            weights = [jnp.ones_like(value), *parts_of(value, 2), *parts_of(var, 2)]
            left.append(
                jnp.concatenate(
                    [jnp.where(in_high, tall(w, HALF), none[:HALF]) for w in weights], axis=0
                )
            )
            right.append(jnp.where(in_low, one, none))
            odd = ((point >> 7) & 1).astype(F32)
            parts = [*parts_of(value * value, 3), *parts_of(var * var, 3), jnp.zeros_like(value)]
            parts.append(parts[-1])
            square.append(
                jnp.concatenate(
                    [p * (1.0 - odd) for p in parts] + [p * odd for p in parts], axis=0
                ).astype(BF16)
            )
        left = jnp.concatenate(left, axis=1)
        right = jnp.concatenate(right, axis=1)
        square = jnp.concatenate(square, axis=1)
        acc[...] += lax.dot_general(left, right, across, preferred_element_type=F32)
        acc_q[...] += lax.dot_general(square, left[:HALF], across, preferred_element_type=F32)

    squares = jnp.concatenate([acc_q[:8, :], acc_q[8:, :]], axis=1)
    for parity in range(2):
        lanes = slice(parity * LANES, (parity + 1) * LANES)
        for y in range(4):
            part = [
                acc[k * HALF + y * OWN : k * HALF + (y + 1) * OWN, lanes] for k in range(5)
            ]
            piece = sums.at[parity, y]
            piece[2 * OWN : 3 * OWN, :] = part[0]
            piece[3 * OWN : 4 * OWN, :] = part[1] + part[2]
            piece[4 * OWN : 5 * OWN, :] = part[3] + part[4]
            piece[5 * OWN :, :] = squares


def looked_up(tables, own_v, ids_col):
    sub = lax.broadcasted_iota(I32, (LANES, LANES), 0)
    lane = lax.broadcasted_iota(I32, (LANES, LANES), 1)
    in_row = (lax.broadcasted_iota(I32, (LANES, 32), 1) == (ids_col >> 7)).astype(F32)
    rows = []
    for table in tables:
        picked = jnp.dot(
            in_row, table[...], precision=lax.Precision.HIGHEST, preferred_element_type=F32
        )
        col = jnp.sum(jnp.where(lane == (ids_col & 127), picked, 0.0), axis=1, keepdims=True)
        rows.append(jnp.sum(jnp.where(sub == lane, col, 0.0), axis=0, keepdims=True))
    return rows


def kernel(
    ens, val, var, pnt, own, mean_tab, var_tab,
    out, post,
    ens_v, val_v, var_v, pnt_v, own_v, mean_v, ivar_v,
    acc, acc_q, sums, from_core, to_chip, from_chip, means, my_lam, lams, scale, to_region, from_region,
    load_sem, core_send, core_recv, chip_send, chip_recv,
    mean_send, mean_recv, lam_send, lam_recv, reg_send, reg_recv,
):
    loads = [
        pltpu.make_async_copy(a, b, load_sem.at[i])
        for i, (a, b) in enumerate(
            (
                (ens, ens_v),
                (pnt, pnt_v),
                (val, val_v),
                (var, var_v),
                (own, own_v),
                (mean_tab, mean_v),
                (var_tab, ivar_v),
            )
        )
    ]
    for load in loads:
        load.start()

    region, member = lax.axis_index("region"), lax.axis_index("member")
    y, core = member // 2, member % 2
    ys = [y, *((y + d) % 4 for d in range(1, 4))]
    others = [2 * ys[d] + c for d in (2, 1, 3) for c in (core, 1 - core)] + [2 * y + 1 - core]
    xs = [8 * ((region // 8 + d) % 4) for d in range(4)]
    zs = [(region % 8 + d) % 8 for d in range(8)]
    far = sorted(
        ((dx, dz) for dx in range(4) for dz in range(8) if dx or dz),
        key=lambda d: -min(d[0], 4 - d[0]) - min(d[1], 8 - d[1]),
    )
    peers = [(xs[dx] + zs[dz], 8 * dx + dz - 1) for dx, dz in far]

    barrier = pltpu.get_barrier_semaphore()
    for peer, _ in peers:
        pl.semaphore_signal(barrier, inc=1, device_id={"region": peer}, device_id_type=MESH)
    for peer in others:
        pl.semaphore_signal(barrier, inc=1, device_id={"member": peer}, device_id_type=MESH)

    for load in loads:
        load.wait()

    point_sums(ens_v, sums)
    histograms(val_v, var_v, pnt_v, acc, acc_q, sums)

    pl.semaphore_wait(barrier, len(peers) + len(others))

    order = (2, 1, 3, 0)
    core_copies = {}
    for d in order:
        core_copies[d] = pltpu.make_async_remote_copy(
            src_ref=sums.at[1 - core, ys[d]],
            dst_ref=from_core.at[d],
            send_sem=core_send.at[d],
            recv_sem=core_recv.at[d],
            device_id={"member": 2 * y + 1 - core},
            device_id_type=MESH,
        )
        core_copies[d].start()
    chip_copies = {}
    for d in order:
        core_copies[d].wait_recv()
        to_chip[d] = sums[core, ys[d]] + from_core[d]
        if d:
            chip_copies[d] = pltpu.make_async_remote_copy(
                src_ref=to_chip.at[d],
                dst_ref=from_chip.at[d - 1],
                send_sem=chip_send.at[d - 1],
                recv_sem=chip_recv.at[d - 1],
                device_id={"member": 2 * ys[d] + core},
                device_id_type=MESH,
            )
            chip_copies[d].start()

    sub = lax.broadcasted_iota(I32, (LANES, LANES), 0)
    lane = lax.broadcasted_iota(I32, (LANES, LANES), 1)
    slot = 2 * (sub & (HALF - 1)) + (sub >> 6)
    ids_col = jnp.sum(
        jnp.where(lane == slot, own_v[...].astype(F32), 0.0), axis=1, keepdims=True
    ).astype(I32)
    prior_mean, prior_var = looked_up((mean_v, ivar_v), own_v, ids_col)
    blocks = [
        (8 * g + (lane >> 4)) * LANES + member * OWN + (lane & (OWN - 1)) == ids_col
        for g in range(4)
    ]

    for d in (1, 3, 2):
        chip_copies[d].wait_recv()

    def summed(k, size=OWN):
        at = slice(k * OWN, k * OWN + size)
        return (to_chip[0, at, :] + from_chip[0, at, :]) + (
            from_chip[1, at, :] + from_chip[2, at, :]
        )

    mean = summed(0) / 80.0
    first = core * HALF + y * OWN
    my_rows = pl.ds(pl.multiple_of(first, OWN), OWN)
    means[my_rows, :] = mean
    mean_copies = []
    for i, peer in enumerate(others):
        mean_copies.append(
            pltpu.make_async_remote_copy(
                src_ref=means.at[my_rows],
                dst_ref=means.at[my_rows],
                send_sem=mean_send.at[i],
                recv_sem=mean_recv.at[i],
                device_id={"member": peer},
                device_id_type=MESH,
            )
        )
        mean_copies[-1].start()

    spread = (summed(1) - 80.0 * mean * mean) / 79.0
    count, value, error, squares = summed(2), summed(3), summed(4), summed(5, 8)
    mine = (
        lax.broadcasted_iota(I32, (OWN, LANES), 1)
        == lax.broadcasted_iota(I32, (OWN, LANES), 0) + first
    )

    def per_slot(x):
        col = jnp.sum(x, axis=1, keepdims=True)
        return jnp.sum(jnp.where(mine, col, 0.0), axis=0, keepdims=True)

    innov_sum = jnp.sum(squares[0:3], axis=0, keepdims=True) + per_slot(
        mean * (count * mean - 2.0 * value)
    )
    error_error = jnp.sum(squares[3:6], axis=0, keepdims=True)
    count_spread = count * spread
    spread_sum = per_slot(count_spread)
    spread_spread = per_slot(count_spread * spread)
    spread_error = per_slot(spread * error)
    error_sum = per_slot(error)
    weight_var = (
        2.0 * prior_mean * prior_mean * (1.0 + spread_spread)
        + 4.0 * prior_mean * spread_error
        + 2.0 * error_error
    )
    lam = jnp.maximum(
        (prior_mean * weight_var + prior_var * spread_sum * (innov_sum - error_sum))
        / (weight_var + prior_var * spread_sum * spread_sum),
        1.0,
    )
    lane_row = lax.broadcasted_iota(I32, (1, LANES), 1)
    my_lam[...] = jnp.where((lane_row >= first) & (lane_row < first + OWN), lam, 0.0)
    lam_copies = []
    for i, peer in enumerate(others):
        lam_copies.append(
            pltpu.make_async_remote_copy(
                src_ref=my_lam,
                dst_ref=lams.at[i],
                send_sem=lam_send.at[i],
                recv_sem=lam_recv.at[i],
                device_id={"member": peer},
                device_id_type=MESH,
            )
        )
        lam_copies[-1].start()
    for copy in lam_copies:
        copy.wait_recv()
    lam_row = my_lam[...]
    for i in range(len(others)):
        lam_row = lam_row + lams[i]
    lam_col = jnp.sum(jnp.where(sub == lane, lam_row, 0.0), axis=1, keepdims=True)

    for g in range(4):
        to_region[g] = jnp.sum(jnp.where(blocks[g], lam_col, 0.0), axis=0, keepdims=True)
    reg_copies = []
    for peer, i in peers:
        reg_copies.append(
            pltpu.make_async_remote_copy(
                src_ref=to_region.at[peer // 8],
                dst_ref=from_region.at[i],
                send_sem=reg_send.at[i],
                recv_sem=reg_recv.at[i],
                device_id={"region": peer},
                device_id_type=MESH,
            )
        )
        reg_copies[-1].start()

    scale[...] = jnp.broadcast_to(jnp.sqrt(lam_col), (LANES, LANES))
    for copy in mean_copies:
        copy.wait_recv()

    @pl.loop(0, 16)
    def _(j):
        for i in range(8):
            at = pl.ds(pl.multiple_of(j * 1024 + i * LANES, LANES), LANES)
            row = pl.ds(HALF * (i % 2) + 4 * j + i // 2, 1)
            m = means[row, :]
            x = ens_v[:, at].astype(F32)
            out[:, at] = (m + scale[row, :] * (x - m)).astype(BF16)

    for copy in reg_copies:
        copy.wait_recv()
    post_row = to_region[region // 8]
    for i in range(len(peers)):
        post_row = post_row + from_region[i]
    turned = pltpu.roll(
        jnp.broadcast_to(post_row, (8, LANES)), (8 - region % 8) * OWN % LANES, 1
    )
    post[...] = turned[0:1, :OWN]

    for copy in (
        *core_copies.values(), *chip_copies.values(), *mean_copies, *lam_copies, *reg_copies
    ):
        copy.wait_send()


def body(ensemble, obs_value, obs_var, obs_point, owned_blocks, infl_mean, infl_var):
    anywhere = pl.BlockSpec(memory_space=pl.ANY)
    vmem = pl.BlockSpec(memory_space=pltpu.VMEM)
    dma = pltpu.SemaphoreType.DMA
    inflated, post = pl.pallas_call(
        kernel,
        out_shape=(pltpu.VMEM(ensemble.shape, BF16), pltpu.VMEM((1, OWN), F32)),
        in_specs=[anywhere] * 7,
        out_specs=(vmem, vmem),
        scratch_shapes=[
            pltpu.VMEM((10, 16384), BF16),
            pltpu.VMEM((32, LANES), F32),
            pltpu.VMEM((32, LANES), F32),
            pltpu.VMEM((32, LANES), I32),
            pltpu.VMEM((1, LANES), I32),
            pltpu.VMEM((32, LANES), F32),
            pltpu.VMEM((32, LANES), F32),
            pltpu.VMEM((5 * HALF, 2 * LANES), F32),
            pltpu.VMEM((16, HALF), F32),
            pltpu.VMEM((2, 4, PIECE, LANES), F32),
            pltpu.VMEM((4, PIECE, LANES), F32),
            pltpu.VMEM((4, PIECE, LANES), F32),
            pltpu.VMEM((3, PIECE, LANES), F32),
            pltpu.VMEM((LANES, LANES), F32),
            pltpu.VMEM((1, LANES), F32),
            pltpu.VMEM((7, 1, LANES), F32),
            pltpu.VMEM((LANES, LANES), F32),
            pltpu.VMEM((4, 1, LANES), F32),
            pltpu.VMEM((31, 1, LANES), F32),
            dma((7,)),
            *[dma((n,)) for n in (4, 3, 7, 7, 31) for _ in range(2)],
        ],
        compiler_params=pltpu.CompilerParams(collective_id=0, has_side_effects=True),
    )(
        ensemble,
        obs_value,
        obs_var,
        obs_point,
        owned_blocks.reshape(1, -1),
        infl_mean.reshape(32, LANES),
        infl_var.reshape(32, LANES),
    )
    return inflated, post.reshape(-1)


def solution(mesh):
    placed = (
        P("member", "region"),
        P(("region", "member"), None),
        P(("region", "member"), None),
        P(("region", "member"), None),
        P("region"),
        P(),
        P(),
    )
    return jax.shard_map(
        body,
        mesh=mesh,
        in_specs=placed,
        out_specs=(P("member", "region"), P(("region", "member"))),
        check_vma=False,
    )
```

```python
import jax
import jax.numpy as jnp
from jax import lax
from jax.experimental import pallas as pl
from jax.experimental.pallas import tpu as pltpu
from jax.sharding import PartitionSpec as P

MESH = pl.DeviceIdType.MESH
F32 = jnp.float32
BF16 = jnp.bfloat16
I32 = jnp.int32
OWN = 16
LANES = 128
HALF = 64
PIECE = 5 * OWN + 8
STEP = 16


def parts_of(x, count):
    parts = []
    for _ in range(count):
        parts.append(x.astype(BF16))
        x = x - parts[-1].astype(F32)
    return [p.astype(F32) for p in parts]


def point_sums(ens_v, sums):
    @pl.loop(0, 16)
    def _(j):
        x = ens_v[:, pl.ds(pl.multiple_of(j * 1024, 1024), 1024)].astype(F32)
        total = jnp.sum(x, axis=0, keepdims=True)
        square = jnp.sum(x * x, axis=0, keepdims=True)
        for i in range(8):
            row = 4 * (j % 4) + i // 2
            piece = sums.at[i % 2, j // 4]
            piece[pl.ds(row, 1), :] = total[:, i * LANES : (i + 1) * LANES]
            piece[pl.ds(OWN + row, 1), :] = square[:, i * LANES : (i + 1) * LANES]


def tall(row, rows):
    same = jnp.broadcast_to(row, (16, LANES)).astype(BF16)
    return jnp.concatenate([same] * (rows // 16), axis=0)


def histograms(val_v, var_v, pnt_v, acc, acc_q, sums):
    across = (((1,), (1,)), ((), ()))
    index = lax.broadcasted_iota(I32, (256, LANES), 0).astype(F32).astype(BF16)
    none, one = jnp.zeros((256, LANES), BF16), jnp.ones((256, LANES), BF16)
    acc[...] = jnp.zeros_like(acc)
    acc_q[...] = jnp.zeros_like(acc_q)

    @pl.loop(0, 32 // STEP)
    def _(step):
        left, right, square = [], [], []
        for i in range(STEP):
            at = pl.ds(step * STEP + i, 1)
            point, value, var = pnt_v[at, :], val_v[at, :], var_v[at, :]
            in_high = index[:HALF] == tall((point >> 8).astype(F32), HALF)
            in_low = index == tall((point & 255).astype(F32), 256)
            weights = [jnp.ones_like(value), *parts_of(value, 2), *parts_of(var, 2)]
            left.append(
                jnp.concatenate(
                    [jnp.where(in_high, tall(w, HALF), none[:HALF]) for w in weights], axis=0
                )
            )
            right.append(jnp.where(in_low, one, none))
            odd = ((point >> 7) & 1).astype(F32)
            parts = [*parts_of(value * value, 3), *parts_of(var * var, 3), jnp.zeros_like(value)]
            parts.append(parts[-1])
            square.append(
                jnp.concatenate(
                    [p * (1.0 - odd) for p in parts] + [p * odd for p in parts], axis=0
                ).astype(BF16)
            )
        left = jnp.concatenate(left, axis=1)
        right = jnp.concatenate(right, axis=1)
        square = jnp.concatenate(square, axis=1)
        acc[...] += lax.dot_general(left, right, across, preferred_element_type=F32)
        acc_q[...] += lax.dot_general(square, left[:HALF], across, preferred_element_type=F32)

    squares = jnp.concatenate([acc_q[:8, :], acc_q[8:, :]], axis=1)
    for parity in range(2):
        lanes = slice(parity * LANES, (parity + 1) * LANES)
        for y in range(4):
            part = [
                acc[k * HALF + y * OWN : k * HALF + (y + 1) * OWN, lanes] for k in range(5)
            ]
            piece = sums.at[parity, y]
            piece[2 * OWN : 3 * OWN, :] = part[0]
            piece[3 * OWN : 4 * OWN, :] = part[1] + part[2]
            piece[4 * OWN : 5 * OWN, :] = part[3] + part[4]
            piece[5 * OWN :, :] = squares


def looked_up(tables, own_v, ids_col):
    sub = lax.broadcasted_iota(I32, (LANES, LANES), 0)
    lane = lax.broadcasted_iota(I32, (LANES, LANES), 1)
    in_row = (lax.broadcasted_iota(I32, (LANES, 32), 1) == (ids_col >> 7)).astype(F32)
    rows = []
    for table in tables:
        picked = jnp.dot(
            in_row, table[...], precision=lax.Precision.HIGHEST, preferred_element_type=F32
        )
        col = jnp.sum(jnp.where(lane == (ids_col & 127), picked, 0.0), axis=1, keepdims=True)
        rows.append(jnp.sum(jnp.where(sub == lane, col, 0.0), axis=0, keepdims=True))
    return rows


def kernel(
    ens, val, var, pnt, own, mean_tab, var_tab,
    out, post,
    ens_v, val_v, var_v, pnt_v, own_v, mean_v, ivar_v,
    acc, acc_q, sums, from_core, to_chip, from_chip, means, my_lam, lams, scale, to_region, from_region,
    load_sem, core_send, core_recv, chip_send, chip_recv,
    mean_send, mean_recv, lam_send, lam_recv, reg_send, reg_recv,
):
    loads = [
        pltpu.make_async_copy(a, b, load_sem.at[i])
        for i, (a, b) in enumerate(
            (
                (ens, ens_v),
                (pnt, pnt_v),
                (val, val_v),
                (var, var_v),
                (own, own_v),
                (mean_tab, mean_v),
                (var_tab, ivar_v),
            )
        )
    ]
    for load in loads:
        load.start()

    region, member = lax.axis_index("region"), lax.axis_index("member")
    y, core = member // 2, member % 2
    ys = [y, *((y + d) % 4 for d in range(1, 4))]
    others = [2 * ys[d] + c for d in (2, 1, 3) for c in (core, 1 - core)] + [2 * y + 1 - core]
    xs = [8 * ((region // 8 + d) % 4) for d in range(4)]
    zs = [(region % 8 + d) % 8 for d in range(8)]
    far = sorted(
        ((dx, dz) for dx in range(4) for dz in range(8) if dx or dz),
        key=lambda d: -min(d[0], 4 - d[0]) - min(d[1], 8 - d[1]),
    )
    peers = [(xs[dx] + zs[dz], 8 * dx + dz - 1) for dx, dz in far]

    barrier = pltpu.get_barrier_semaphore()
    for peer, _ in peers:
        pl.semaphore_signal(barrier, inc=1, device_id={"region": peer}, device_id_type=MESH)
    for peer in others:
        pl.semaphore_signal(barrier, inc=1, device_id={"member": peer}, device_id_type=MESH)

    for load in loads:
        load.wait()

    point_sums(ens_v, sums)
    histograms(val_v, var_v, pnt_v, acc, acc_q, sums)

    pl.semaphore_wait(barrier, len(peers) + len(others))

    order = (2, 1, 3, 0)
    core_copies = {}
    for d in order:
        core_copies[d] = pltpu.make_async_remote_copy(
            src_ref=sums.at[1 - core, ys[d]],
            dst_ref=from_core.at[d],
            send_sem=core_send.at[d],
            recv_sem=core_recv.at[d],
            device_id={"member": 2 * y + 1 - core},
            device_id_type=MESH,
        )
        core_copies[d].start()
    chip_copies = {}
    for d in order:
        core_copies[d].wait_recv()
        to_chip[d] = sums[core, ys[d]] + from_core[d]
        if d:
            chip_copies[d] = pltpu.make_async_remote_copy(
                src_ref=to_chip.at[d],
                dst_ref=from_chip.at[d - 1],
                send_sem=chip_send.at[d - 1],
                recv_sem=chip_recv.at[d - 1],
                device_id={"member": 2 * ys[d] + core},
                device_id_type=MESH,
            )
            chip_copies[d].start()

    sub = lax.broadcasted_iota(I32, (LANES, LANES), 0)
    lane = lax.broadcasted_iota(I32, (LANES, LANES), 1)
    slot = 2 * (sub & (HALF - 1)) + (sub >> 6)
    ids_col = jnp.sum(
        jnp.where(lane == slot, own_v[...].astype(F32), 0.0), axis=1, keepdims=True
    ).astype(I32)
    prior_mean, prior_var = looked_up((mean_v, ivar_v), own_v, ids_col)
    blocks = [
        (8 * g + (lane >> 4)) * LANES + member * OWN + (lane & (OWN - 1)) == ids_col
        for g in range(4)
    ]

    for d in (1, 3, 2):
        chip_copies[d].wait_recv()

    def summed(k, size=OWN):
        at = slice(k * OWN, k * OWN + size)
        return (to_chip[0, at, :] + from_chip[0, at, :]) + (
            from_chip[1, at, :] + from_chip[2, at, :]
        )

    mean = summed(0) / 80.0
    first = core * HALF + y * OWN
    my_rows = pl.ds(pl.multiple_of(first, OWN), OWN)
    means[my_rows, :] = mean
    spread = (summed(1) - 80.0 * mean * mean) / 79.0
    count, value, error, squares = summed(2), summed(3), summed(4), summed(5, 8)
    mine = (
        lax.broadcasted_iota(I32, (OWN, LANES), 1)
        == lax.broadcasted_iota(I32, (OWN, LANES), 0) + first
    )

    def per_slot(x):
        col = jnp.sum(x, axis=1, keepdims=True)
        return jnp.sum(jnp.where(mine, col, 0.0), axis=0, keepdims=True)

    innov_sum = jnp.sum(squares[0:3], axis=0, keepdims=True) + per_slot(
        mean * (count * mean - 2.0 * value)
    )
    error_error = jnp.sum(squares[3:6], axis=0, keepdims=True)
    count_spread = count * spread
    spread_sum = per_slot(count_spread)
    spread_spread = per_slot(count_spread * spread)
    spread_error = per_slot(spread * error)
    error_sum = per_slot(error)
    weight_var = (
        2.0 * prior_mean * prior_mean * (1.0 + spread_spread)
        + 4.0 * prior_mean * spread_error
        + 2.0 * error_error
    )
    lam = jnp.maximum(
        (prior_mean * weight_var + prior_var * spread_sum * (innov_sum - error_sum))
        / (weight_var + prior_var * spread_sum * spread_sum),
        1.0,
    )
    lane_row = lax.broadcasted_iota(I32, (1, LANES), 1)
    my_lam[...] = jnp.where((lane_row >= first) & (lane_row < first + OWN), lam, 0.0)
    lam_copies = []
    for i, peer in enumerate(others):
        lam_copies.append(
            pltpu.make_async_remote_copy(
                src_ref=my_lam,
                dst_ref=lams.at[i],
                send_sem=lam_send.at[i],
                recv_sem=lam_recv.at[i],
                device_id={"member": peer},
                device_id_type=MESH,
            )
        )
        lam_copies[-1].start()
    mean_copies = []
    for i, peer in enumerate(others):
        mean_copies.append(
            pltpu.make_async_remote_copy(
                src_ref=means.at[my_rows],
                dst_ref=means.at[my_rows],
                send_sem=mean_send.at[i],
                recv_sem=mean_recv.at[i],
                device_id={"member": peer},
                device_id_type=MESH,
            )
        )
        mean_copies[-1].start()

    for copy in lam_copies:
        copy.wait_recv()
    lam_row = my_lam[...]
    for i in range(len(others)):
        lam_row = lam_row + lams[i]
    lam_col = jnp.sum(jnp.where(sub == lane, lam_row, 0.0), axis=1, keepdims=True)

    for g in range(4):
        to_region[g] = jnp.sum(jnp.where(blocks[g], lam_col, 0.0), axis=0, keepdims=True)
    reg_copies = []
    for peer, i in peers:
        reg_copies.append(
            pltpu.make_async_remote_copy(
                src_ref=to_region.at[peer // 8],
                dst_ref=from_region.at[i],
                send_sem=reg_send.at[i],
                recv_sem=reg_recv.at[i],
                device_id={"region": peer},
                device_id_type=MESH,
            )
        )
        reg_copies[-1].start()

    scale[...] = jnp.broadcast_to(jnp.sqrt(lam_col), (LANES, LANES))
    for copy in mean_copies:
        copy.wait_recv()

    @pl.loop(0, 16)
    def _(j):
        for i in range(8):
            at = pl.ds(pl.multiple_of(j * 1024 + i * LANES, LANES), LANES)
            row = pl.ds(HALF * (i % 2) + 4 * j + i // 2, 1)
            m = means[row, :]
            x = ens_v[:, at].astype(F32)
            out[:, at] = (m + scale[row, :] * (x - m)).astype(BF16)

    for copy in reg_copies:
        copy.wait_recv()
    post_row = to_region[region // 8]
    for i in range(len(peers)):
        post_row = post_row + from_region[i]
    turned = pltpu.roll(
        jnp.broadcast_to(post_row, (8, LANES)), (8 - region % 8) * OWN % LANES, 1
    )
    post[...] = turned[0:1, :OWN]

    for copy in (
        *core_copies.values(), *chip_copies.values(), *mean_copies, *lam_copies, *reg_copies
    ):
        copy.wait_send()


def written(a, b, a_out, b_out, sem):
    copies = [
        pltpu.make_async_copy(a, a_out, sem.at[0]),
        pltpu.make_async_copy(b, b_out, sem.at[1]),
    ]
    for copy in copies:
        copy.start()
    for copy in copies:
        copy.wait()


def body(ensemble, obs_value, obs_var, obs_point, owned_blocks, infl_mean, infl_var):
    anywhere = pl.BlockSpec(memory_space=pl.ANY)
    vmem = pl.BlockSpec(memory_space=pltpu.VMEM)
    dma = pltpu.SemaphoreType.DMA
    inflated, post = pl.pallas_call(
        kernel,
        out_shape=(pltpu.VMEM(ensemble.shape, BF16), pltpu.VMEM((1, OWN), F32)),
        in_specs=[anywhere] * 7,
        out_specs=(vmem, vmem),
        scratch_shapes=[
            pltpu.VMEM((10, 16384), BF16),
            pltpu.VMEM((32, LANES), F32),
            pltpu.VMEM((32, LANES), F32),
            pltpu.VMEM((32, LANES), I32),
            pltpu.VMEM((1, LANES), I32),
            pltpu.VMEM((32, LANES), F32),
            pltpu.VMEM((32, LANES), F32),
            pltpu.VMEM((5 * HALF, 2 * LANES), F32),
            pltpu.VMEM((16, HALF), F32),
            pltpu.VMEM((2, 4, PIECE, LANES), F32),
            pltpu.VMEM((4, PIECE, LANES), F32),
            pltpu.VMEM((4, PIECE, LANES), F32),
            pltpu.VMEM((3, PIECE, LANES), F32),
            pltpu.VMEM((LANES, LANES), F32),
            pltpu.VMEM((1, LANES), F32),
            pltpu.VMEM((7, 1, LANES), F32),
            pltpu.VMEM((LANES, LANES), F32),
            pltpu.VMEM((4, 1, LANES), F32),
            pltpu.VMEM((31, 1, LANES), F32),
            dma((7,)),
            *[dma((n,)) for n in (4, 3, 7, 7, 31) for _ in range(2)],
        ],
        compiler_params=pltpu.CompilerParams(collective_id=0, has_side_effects=True),
    )(
        ensemble,
        obs_value,
        obs_var,
        obs_point,
        owned_blocks.reshape(1, -1),
        infl_mean.reshape(32, LANES),
        infl_var.reshape(32, LANES),
    )
    inflated, post = pl.pallas_call(
        written,
        out_shape=(
            jax.ShapeDtypeStruct(ensemble.shape, BF16),
            jax.ShapeDtypeStruct((1, OWN), F32),
        ),
        in_specs=(vmem, vmem),
        out_specs=(anywhere, anywhere),
        scratch_shapes=[dma((2,))],
    )(
        pltpu.with_memory_space_constraint(inflated, pltpu.VMEM),
        pltpu.with_memory_space_constraint(post, pltpu.VMEM),
    )
    return inflated, post.reshape(-1)


def solution(mesh):
    placed = (
        P("member", "region"),
        P(("region", "member"), None),
        P(("region", "member"), None),
        P(("region", "member"), None),
        P("region"),
        P(),
        P(),
    )
    return jax.shard_map(
        body,
        mesh=mesh,
        in_specs=placed,
        out_specs=(P("member", "region"), P(("region", "member"))),
        check_vma=False,
    )
```

```python
import jax
import jax.numpy as jnp
from jax import lax
from jax.experimental import pallas as pl
from jax.experimental.pallas import tpu as pltpu
from jax.sharding import PartitionSpec as P

MESH = pl.DeviceIdType.MESH
F32 = jnp.float32
BF16 = jnp.bfloat16
I32 = jnp.int32
OWN = 16
LANES = 128
HALF = 64
PIECE = 5 * OWN + 8
STEP = 16


def parts_of(x, count):
    parts = []
    for _ in range(count):
        parts.append(x.astype(BF16))
        x = x - parts[-1].astype(F32)
    return [p.astype(F32) for p in parts]


def point_sums(ens_v, sums):
    @pl.loop(0, 16)
    def _(j):
        x = ens_v[:, pl.ds(pl.multiple_of(j * 1024, 1024), 1024)].astype(F32)
        total = jnp.sum(x, axis=0, keepdims=True)
        square = jnp.sum(x * x, axis=0, keepdims=True)
        for i in range(8):
            row = 4 * (j % 4) + i // 2
            piece = sums.at[i % 2, j // 4]
            piece[pl.ds(row, 1), :] = total[:, i * LANES : (i + 1) * LANES]
            piece[pl.ds(OWN + row, 1), :] = square[:, i * LANES : (i + 1) * LANES]


def tall(row, rows):
    same = jnp.broadcast_to(row, (16, LANES)).astype(BF16)
    return jnp.concatenate([same] * (rows // 16), axis=0)


def histograms(val_v, var_v, pnt_v, acc, acc_q, sums):
    across = (((1,), (1,)), ((), ()))
    index = lax.broadcasted_iota(I32, (256, LANES), 0).astype(F32).astype(BF16)
    none, one = jnp.zeros((256, LANES), BF16), jnp.ones((256, LANES), BF16)
    acc[...] = jnp.zeros_like(acc)
    acc_q[...] = jnp.zeros_like(acc_q)

    @pl.loop(0, 32 // STEP)
    def _(step):
        left, right, square = [], [], []
        for i in range(STEP):
            at = pl.ds(step * STEP + i, 1)
            point, value, var = pnt_v[at, :], val_v[at, :], var_v[at, :]
            in_high = index[:HALF] == tall((point >> 8).astype(F32), HALF)
            in_low = index == tall((point & 255).astype(F32), 256)
            weights = [jnp.ones_like(value), *parts_of(value, 2), *parts_of(var, 2)]
            left.append(
                jnp.concatenate(
                    [jnp.where(in_high, tall(w, HALF), none[:HALF]) for w in weights], axis=0
                )
            )
            right.append(jnp.where(in_low, one, none))
            odd = ((point >> 7) & 1).astype(F32)
            parts = [*parts_of(value * value, 3), *parts_of(var * var, 3), jnp.zeros_like(value)]
            parts.append(parts[-1])
            square.append(
                jnp.concatenate(
                    [p * (1.0 - odd) for p in parts] + [p * odd for p in parts], axis=0
                ).astype(BF16)
            )
        left = jnp.concatenate(left, axis=1)
        right = jnp.concatenate(right, axis=1)
        square = jnp.concatenate(square, axis=1)
        acc[...] += lax.dot_general(left, right, across, preferred_element_type=F32)
        acc_q[...] += lax.dot_general(square, left[:HALF], across, preferred_element_type=F32)

    squares = jnp.concatenate([acc_q[:8, :], acc_q[8:, :]], axis=1)
    for parity in range(2):
        lanes = slice(parity * LANES, (parity + 1) * LANES)
        for y in range(4):
            part = [
                acc[k * HALF + y * OWN : k * HALF + (y + 1) * OWN, lanes] for k in range(5)
            ]
            piece = sums.at[parity, y]
            piece[2 * OWN : 3 * OWN, :] = part[0]
            piece[3 * OWN : 4 * OWN, :] = part[1] + part[2]
            piece[4 * OWN : 5 * OWN, :] = part[3] + part[4]
            piece[5 * OWN :, :] = squares


def looked_up(tables, ids_col):
    slots = ids_col.shape[0]
    lane = lax.broadcasted_iota(I32, (slots, LANES), 1)
    in_row = (lax.broadcasted_iota(I32, (slots, 32), 1) == (ids_col >> 7)).astype(F32)
    cols = []
    for table in tables:
        picked = jnp.dot(
            in_row, table[...], precision=lax.Precision.HIGHEST, preferred_element_type=F32
        )
        cols.append(
            jnp.sum(jnp.where(lane == (ids_col & 127), picked, 0.0), axis=1, keepdims=True)
        )
    return cols


def kernel(
    ens, val, var, pnt, own, mean_tab, var_tab,
    out, post,
    ens_v, val_v, var_v, pnt_v, own_v, mean_v, ivar_v,
    acc, acc_q, sums, from_core, to_chip, from_chip, means, my_lam, lams, scale, to_region, from_region,
    load_sem, core_send, core_recv, chip_send, chip_recv,
    mean_send, mean_recv, lam_send, lam_recv, reg_send, reg_recv,
):
    loads = [
        pltpu.make_async_copy(a, b, load_sem.at[i])
        for i, (a, b) in enumerate(
            (
                (ens, ens_v),
                (pnt, pnt_v),
                (val, val_v),
                (var, var_v),
                (own, own_v),
                (mean_tab, mean_v),
                (var_tab, ivar_v),
            )
        )
    ]
    for load in loads:
        load.start()

    region, member = lax.axis_index("region"), lax.axis_index("member")
    y, core = member // 2, member % 2
    ys = [y, *((y + d) % 4 for d in range(1, 4))]
    others = [2 * ys[d] + c for d in (2, 1, 3) for c in (core, 1 - core)] + [2 * y + 1 - core]
    xs = [8 * ((region // 8 + d) % 4) for d in range(4)]
    zs = [(region % 8 + d) % 8 for d in range(8)]
    far = sorted(
        ((dx, dz) for dx in range(4) for dz in range(8) if dx or dz),
        key=lambda d: -min(d[0], 4 - d[0]) - min(d[1], 8 - d[1]),
    )
    regions = [xs[dx] + zs[dz] for dx, dz in far]
    members = [2 * ys[d] + c for d in range(4) for c in (core, 1 - core)]
    apart = sorted(
        (
            (-sum(min(a, n - a) for a, n in zip(d[:3], (4, 8, 4))), d)
            for d in ((dx, dz, dy, c) for dx in range(4) for dz in range(8) for dy in range(4) for c in range(2))
            if any(d)
        )
    )
    peers = [(xs[dx] + zs[dz], members[2 * dy + c]) for _, (dx, dz, dy, c) in apart]

    barrier = pltpu.get_barrier_semaphore()
    for peer in regions:
        pl.semaphore_signal(barrier, inc=1, device_id={"region": peer}, device_id_type=MESH)
    for peer in others:
        pl.semaphore_signal(barrier, inc=1, device_id={"member": peer}, device_id_type=MESH)

    for load in loads:
        load.wait()

    point_sums(ens_v, sums)
    histograms(val_v, var_v, pnt_v, acc, acc_q, sums)

    pl.semaphore_wait(barrier, len(regions) + len(others))

    order = (2, 1, 3, 0)
    core_copies = {}
    for d in order:
        core_copies[d] = pltpu.make_async_remote_copy(
            src_ref=sums.at[1 - core, ys[d]],
            dst_ref=from_core.at[d],
            send_sem=core_send.at[d],
            recv_sem=core_recv.at[d],
            device_id={"member": 2 * y + 1 - core},
            device_id_type=MESH,
        )
        core_copies[d].start()
    chip_copies = {}
    for d in order:
        core_copies[d].wait_recv()
        to_chip[d] = sums[core, ys[d]] + from_core[d]
        if d:
            chip_copies[d] = pltpu.make_async_remote_copy(
                src_ref=to_chip.at[d],
                dst_ref=from_chip.at[d - 1],
                send_sem=chip_send.at[d - 1],
                recv_sem=chip_recv.at[d - 1],
                device_id={"member": 2 * ys[d] + core},
                device_id_type=MESH,
            )
            chip_copies[d].start()

    sub = lax.broadcasted_iota(I32, (OWN, LANES), 0)
    lane = lax.broadcasted_iota(I32, (OWN, LANES), 1)
    ids_col = jnp.sum(
        jnp.where(lane == 2 * (OWN * y + sub) + core, own_v[...].astype(F32), 0.0),
        axis=1,
        keepdims=True,
    ).astype(I32)
    prior_mean, prior_var = looked_up((mean_v, ivar_v), ids_col)
    in_block = lane == (ids_col & 127)

    for d in (1, 3, 2):
        chip_copies[d].wait_recv()

    def summed(k, size=OWN):
        at = slice(k * OWN, k * OWN + size)
        return (to_chip[0, at, :] + from_chip[0, at, :]) + (
            from_chip[1, at, :] + from_chip[2, at, :]
        )

    mean = summed(0) / 80.0
    first = core * HALF + y * OWN
    my_rows = pl.ds(pl.multiple_of(first, OWN), OWN)
    means[my_rows, :] = mean
    spread = (summed(1) - 80.0 * mean * mean) / 79.0
    count, value, error, squares = summed(2), summed(3), summed(4), summed(5, 8)
    mine = lane == sub + first

    def per_slot(x):
        return jnp.sum(x, axis=1, keepdims=True)

    innov_sum = per_slot(
        jnp.where(mine, jnp.sum(squares[0:3], axis=0, keepdims=True), 0.0)
        + mean * (count * mean - 2.0 * value)
    )
    error_error = per_slot(jnp.where(mine, jnp.sum(squares[3:6], axis=0, keepdims=True), 0.0))
    count_spread = count * spread
    spread_sum = per_slot(count_spread)
    spread_spread = per_slot(count_spread * spread)
    spread_error = per_slot(spread * error)
    error_sum = per_slot(error)
    weight_var = (
        2.0 * prior_mean * prior_mean * (1.0 + spread_spread)
        + 4.0 * prior_mean * spread_error
        + 2.0 * error_error
    )
    lam = jnp.maximum(
        (prior_mean * weight_var + prior_var * spread_sum * (innov_sum - error_sum))
        / (weight_var + prior_var * spread_sum * spread_sum),
        1.0,
    )
    placed = jnp.where(in_block, lam, 0.0)
    for r in range(32):
        to_region[r] = jnp.sum(
            jnp.where((ids_col >> 7) == r, placed, 0.0), axis=0, keepdims=True
        )
    my_lam[...] = jnp.sum(jnp.where(mine, lam, 0.0), axis=0, keepdims=True)

    def to_all(some):
        for i, (peer, dest) in some:
            pltpu.make_async_remote_copy(
                src_ref=to_region.at[peer],
                dst_ref=from_region.at[i],
                send_sem=reg_send,
                recv_sem=reg_recv,
                device_id={"region": peer, "member": dest},
                device_id_type=MESH,
            ).start()

    everyone = list(enumerate(peers))
    to_all(everyone[:96])
    lam_copies = []
    for i, peer in enumerate(others):
        lam_copies.append(
            pltpu.make_async_remote_copy(
                src_ref=my_lam,
                dst_ref=lams.at[i],
                send_sem=lam_send.at[i],
                recv_sem=lam_recv.at[i],
                device_id={"member": peer},
                device_id_type=MESH,
            )
        )
        lam_copies[-1].start()
    mean_copies = []
    for i, peer in enumerate(others):
        mean_copies.append(
            pltpu.make_async_remote_copy(
                src_ref=means.at[my_rows],
                dst_ref=means.at[my_rows],
                send_sem=mean_send.at[i],
                recv_sem=mean_recv.at[i],
                device_id={"member": peer},
                device_id_type=MESH,
            )
        )
        mean_copies[-1].start()

    to_all(everyone[96:])
    for copy in lam_copies:
        copy.wait_recv()
    lam_row = my_lam[...]
    for i in range(len(others)):
        lam_row = lam_row + lams[i]
    eye = lax.broadcasted_iota(I32, (LANES, LANES), 0) == lax.broadcasted_iota(
        I32, (LANES, LANES), 1
    )
    lam_col = jnp.sum(jnp.where(eye, lam_row, 0.0), axis=1, keepdims=True)
    scale[...] = jnp.broadcast_to(jnp.sqrt(lam_col), (LANES, LANES))
    for copy in mean_copies:
        copy.wait_recv()

    @pl.loop(0, 16)
    def _(j):
        for i in range(8):
            at = pl.ds(pl.multiple_of(j * 1024 + i * LANES, LANES), LANES)
            row = pl.ds(HALF * (i % 2) + 4 * j + i // 2, 1)
            m = means[row, :]
            x = ens_v[:, at].astype(F32)
            out[:, at] = (m + scale[row, :] * (x - m)).astype(BF16)

    arrived = pltpu.make_async_remote_copy(
        src_ref=from_region,
        dst_ref=from_region,
        send_sem=reg_send,
        recv_sem=reg_recv,
        device_id={"member": others[0]},
        device_id_type=MESH,
    )
    arrived.wait_recv()
    post_row = to_region[region] + jnp.sum(from_region[...], axis=0)
    turned = pltpu.roll(jnp.broadcast_to(post_row, (8, LANES)), (8 - member) * OWN % LANES, 1)
    post[...] = turned[0:1, :OWN]

    for copy in (
        *core_copies.values(), *chip_copies.values(), *mean_copies, *lam_copies, arrived
    ):
        copy.wait_send()


def written(a, b, a_out, b_out, sem):
    copies = [
        pltpu.make_async_copy(a, a_out, sem.at[0]),
        pltpu.make_async_copy(b, b_out, sem.at[1]),
    ]
    for copy in copies:
        copy.start()
    for copy in copies:
        copy.wait()


def body(ensemble, obs_value, obs_var, obs_point, owned_blocks, infl_mean, infl_var):
    anywhere = pl.BlockSpec(memory_space=pl.ANY)
    vmem = pl.BlockSpec(memory_space=pltpu.VMEM)
    dma = pltpu.SemaphoreType.DMA
    inflated, post = pl.pallas_call(
        kernel,
        out_shape=(pltpu.VMEM(ensemble.shape, BF16), pltpu.VMEM((1, OWN), F32)),
        in_specs=[anywhere] * 7,
        out_specs=(vmem, vmem),
        scratch_shapes=[
            pltpu.VMEM((10, 16384), BF16),
            pltpu.VMEM((32, LANES), F32),
            pltpu.VMEM((32, LANES), F32),
            pltpu.VMEM((32, LANES), I32),
            pltpu.VMEM((1, LANES), I32),
            pltpu.VMEM((32, LANES), F32),
            pltpu.VMEM((32, LANES), F32),
            pltpu.VMEM((5 * HALF, 2 * LANES), F32),
            pltpu.VMEM((16, HALF), F32),
            pltpu.VMEM((2, 4, PIECE, LANES), F32),
            pltpu.VMEM((4, PIECE, LANES), F32),
            pltpu.VMEM((4, PIECE, LANES), F32),
            pltpu.VMEM((3, PIECE, LANES), F32),
            pltpu.VMEM((LANES, LANES), F32),
            pltpu.VMEM((1, LANES), F32),
            pltpu.VMEM((7, 1, LANES), F32),
            pltpu.VMEM((LANES, LANES), F32),
            pltpu.VMEM((32, 1, LANES), F32),
            pltpu.VMEM((255, 1, LANES), F32),
            dma((7,)),
            *[dma((n,)) for n in (4, 3, 7, 7) for _ in range(2)],
            dma,
            dma,
        ],
        compiler_params=pltpu.CompilerParams(collective_id=0, has_side_effects=True),
    )(
        ensemble,
        obs_value,
        obs_var,
        obs_point,
        owned_blocks.reshape(1, -1),
        infl_mean.reshape(32, LANES),
        infl_var.reshape(32, LANES),
    )
    inflated, post = pl.pallas_call(
        written,
        out_shape=(
            jax.ShapeDtypeStruct(ensemble.shape, BF16),
            jax.ShapeDtypeStruct((1, OWN), F32),
        ),
        in_specs=(vmem, vmem),
        out_specs=(anywhere, anywhere),
        scratch_shapes=[dma((2,))],
    )(
        pltpu.with_memory_space_constraint(inflated, pltpu.VMEM),
        pltpu.with_memory_space_constraint(post, pltpu.VMEM),
    )
    return inflated, post.reshape(-1)


def solution(mesh):
    placed = (
        P("member", "region"),
        P(("region", "member"), None),
        P(("region", "member"), None),
        P(("region", "member"), None),
        P("region"),
        P(),
        P(),
    )
    return jax.shard_map(
        body,
        mesh=mesh,
        in_specs=placed,
        out_specs=(P("member", "region"), P(("region", "member"))),
        check_vma=False,
    )
```

```python
import jax
import jax.numpy as jnp
from jax import lax
from jax.experimental import pallas as pl
from jax.experimental.pallas import tpu as pltpu
from jax.sharding import PartitionSpec as P

MESH = pl.DeviceIdType.MESH
F32 = jnp.float32
BF16 = jnp.bfloat16
I32 = jnp.int32
OWN = 16
LANES = 128
HALF = 64
POINTS = 2 * OWN
COUNTS = 3 * OWN + 8
STEP = 16


def parts_of(x, count):
    parts = []
    for _ in range(count):
        parts.append(x.astype(BF16))
        x = x - parts[-1].astype(F32)
    return [p.astype(F32) for p in parts]


def point_sums(ens_v, sums):
    @pl.loop(0, 16)
    def _(j):
        x = ens_v[:, pl.ds(pl.multiple_of(j * 1024, 1024), 1024)].astype(F32)
        total = jnp.sum(x, axis=0, keepdims=True)
        square = jnp.sum(x * x, axis=0, keepdims=True)
        for i in range(8):
            row = 4 * (j % 4) + i // 2
            piece = sums.at[i % 2, j // 4]
            piece[pl.ds(row, 1), :] = total[:, i * LANES : (i + 1) * LANES]
            piece[pl.ds(OWN + row, 1), :] = square[:, i * LANES : (i + 1) * LANES]


def tall(row, rows):
    same = jnp.broadcast_to(row, (16, LANES)).astype(BF16)
    return jnp.concatenate([same] * (rows // 16), axis=0)


def histograms(val_v, var_v, pnt_v, acc, acc_q, counts):
    across = (((1,), (1,)), ((), ()))
    index = lax.broadcasted_iota(I32, (256, LANES), 0).astype(F32).astype(BF16)
    none, one = jnp.zeros((256, LANES), BF16), jnp.ones((256, LANES), BF16)
    acc[...] = jnp.zeros_like(acc)
    acc_q[...] = jnp.zeros_like(acc_q)

    @pl.loop(0, 32 // STEP)
    def _(step):
        left, right, square = [], [], []
        for i in range(STEP):
            at = pl.ds(step * STEP + i, 1)
            point, value, var = pnt_v[at, :], val_v[at, :], var_v[at, :]
            in_high = index[:HALF] == tall((point >> 8).astype(F32), HALF)
            in_low = index == tall((point & 255).astype(F32), 256)
            weights = [jnp.ones_like(value), *parts_of(value, 2), *parts_of(var, 2)]
            left.append(
                jnp.concatenate(
                    [jnp.where(in_high, tall(w, HALF), none[:HALF]) for w in weights], axis=0
                )
            )
            right.append(jnp.where(in_low, one, none))
            odd = ((point >> 7) & 1).astype(F32)
            parts = [*parts_of(value * value, 3), *parts_of(var * var, 3), jnp.zeros_like(value)]
            parts.append(parts[-1])
            square.append(
                jnp.concatenate(
                    [p * (1.0 - odd) for p in parts] + [p * odd for p in parts], axis=0
                ).astype(BF16)
            )
        left = jnp.concatenate(left, axis=1)
        right = jnp.concatenate(right, axis=1)
        square = jnp.concatenate(square, axis=1)
        acc[...] += lax.dot_general(left, right, across, preferred_element_type=F32)
        acc_q[...] += lax.dot_general(square, left[:HALF], across, preferred_element_type=F32)

    squares = jnp.concatenate([acc_q[:8, :], acc_q[8:, :]], axis=1)
    for parity in range(2):
        lanes = slice(parity * LANES, (parity + 1) * LANES)
        for y in range(4):
            part = [
                acc[k * HALF + y * OWN : k * HALF + (y + 1) * OWN, lanes] for k in range(5)
            ]
            piece = counts.at[parity, y]
            piece[:OWN, :] = part[0]
            piece[OWN : 2 * OWN, :] = part[1] + part[2]
            piece[2 * OWN : 3 * OWN, :] = part[3] + part[4]
            piece[3 * OWN :, :] = squares


def looked_up(tables, ids_col):
    slots = ids_col.shape[0]
    lane = lax.broadcasted_iota(I32, (slots, LANES), 1)
    in_row = (lax.broadcasted_iota(I32, (slots, 32), 1) == (ids_col >> 7)).astype(F32)
    cols = []
    for table in tables:
        picked = jnp.dot(
            in_row, table[...], precision=lax.Precision.HIGHEST, preferred_element_type=F32
        )
        cols.append(
            jnp.sum(jnp.where(lane == (ids_col & 127), picked, 0.0), axis=1, keepdims=True)
        )
    return cols


def kernel(
    ens, val, var, pnt, own, mean_tab, var_tab,
    out, post,
    ens_v, val_v, var_v, pnt_v, own_v, mean_v, ivar_v,
    acc, acc_q, sums, counts, sums_core, counts_core, sums_to, counts_to, sums_chip, counts_chip, means, my_lam, lams, scale, to_region, from_region,
    load_sem, line_sem, all_sem, core_send, core_recv, chip_send, chip_recv,
    mean_send, mean_recv, lam_send, lam_recv, reg_send, reg_recv,
):
    loads = [
        pltpu.make_async_copy(a, b, load_sem.at[i])
        for i, (a, b) in enumerate(
            (
                (pnt, pnt_v),
                (val, val_v),
                (var, var_v),
                (ens, ens_v),
                (own, own_v),
                (mean_tab, mean_v),
                (var_tab, ivar_v),
            )
        )
    ]
    for load in loads:
        load.start()
    from_region[255:256, :] = jnp.zeros((1, LANES), F32)

    region, member = lax.axis_index("region"), lax.axis_index("member")
    y, core = member // 2, member % 2
    ys = [y, *((y + d) % 4 for d in range(1, 4))]
    others = [2 * ys[d] + c for d in (2, 1, 3) for c in (core, 1 - core)] + [2 * y + 1 - core]
    xs = [8 * ((region // 8 + d) % 4) for d in range(4)]
    zs = [(region % 8 + d) % 8 for d in range(8)]
    along_x = [xs[d] + zs[0] for d in (2, 1, 3)]
    along_z = [xs[0] + zs[d] for d in (4, 3, 5, 2, 6, 1, 7)]
    members = [2 * ys[d] + c for d in range(4) for c in (core, 1 - core)]
    apart = sorted(
        (
            (-sum(min(a, n - a) for a, n in zip(d[:3], (4, 8, 4))), d)
            for d in ((dx, dz, dy, c) for dx in range(4) for dz in range(8) for dy in range(4) for c in range(2))
            if any(d)
        )
    )
    peers = [(xs[dx] + zs[dz], members[2 * dy + c]) for _, (dx, dz, dy, c) in apart]

    barrier = pltpu.get_barrier_semaphore()
    for peer in others:
        pl.semaphore_signal(barrier, inc=1, device_id={"member": peer}, device_id_type=MESH)
    for peer in (*along_x, *along_z[3:]):
        pl.semaphore_signal(barrier, inc=1, device_id={"region": peer}, device_id_type=MESH)

    for load in loads[:3]:
        load.wait()
    histograms(val_v, var_v, pnt_v, acc, acc_q, counts)

    pl.semaphore_wait(barrier, len(others) + len(along_x) + 4)

    order = (2, 1, 3, 0)
    def core_copy(k, d):
        return pltpu.make_async_remote_copy(
            src_ref=(sums, counts)[k].at[1 - core, ys[d]],
            dst_ref=(sums_core, counts_core)[k].at[d],
            send_sem=core_send.at[4 * k + d],
            recv_sem=core_recv.at[4 * k + d],
            device_id={"member": 2 * y + 1 - core},
            device_id_type=MESH,
        )

    def chip_copy(k, d):
        return pltpu.make_async_remote_copy(
            src_ref=(sums_to, counts_to)[k].at[d],
            dst_ref=(sums_chip, counts_chip)[k].at[d - 1],
            send_sem=chip_send.at[3 * k + d - 1],
            recv_sem=chip_recv.at[3 * k + d - 1],
            device_id={"member": 2 * ys[d] + core},
            device_id_type=MESH,
        )

    def pass_on(k):
        own, came, total = ((sums, sums_core, sums_to), (counts, counts_core, counts_to))[k]
        for d in order:
            core_copy(k, d).wait_recv()
            total[d] = own[core, ys[d]] + came[d]
            if d:
                chip_copy(k, d).start()

    for d in order:
        core_copy(1, d).start()
    for peer in (*along_x, *along_z[3:5]):
        pl.semaphore_signal(line_sem, inc=1, device_id={"region": peer}, device_id_type=MESH)
    for load in loads[3:]:
        load.wait()
    point_sums(ens_v, sums)
    for d in order:
        core_copy(0, d).start()
    pass_on(1)
    pass_on(0)
    pl.semaphore_wait(line_sem, len(along_x) + 2)
    for peer in along_z:
        pl.semaphore_signal(all_sem, inc=1, device_id={"region": peer}, device_id_type=MESH)

    sub = lax.broadcasted_iota(I32, (OWN, LANES), 0)
    lane = lax.broadcasted_iota(I32, (OWN, LANES), 1)
    ids_col = jnp.sum(
        jnp.where(lane == 2 * (OWN * y + sub) + core, own_v[...].astype(F32), 0.0),
        axis=1,
        keepdims=True,
    ).astype(I32)
    prior_mean, prior_var = looked_up((mean_v, ivar_v), ids_col)
    in_block = lane == (ids_col & 127)

    for k in (1, 0):
        for d in (1, 3, 2):
            chip_copy(k, d).wait_recv()

    def summed(total, came, k, size=OWN):
        at = slice(k * OWN, k * OWN + size)
        return (total[0, at, :] + came[0, at, :]) + (came[1, at, :] + came[2, at, :])

    mean = summed(sums_to, sums_chip, 0) / 80.0
    first = core * HALF + y * OWN
    my_rows = pl.ds(pl.multiple_of(first, OWN), OWN)
    means[my_rows, :] = mean
    spread = (summed(sums_to, sums_chip, 1) - 80.0 * mean * mean) / 79.0
    count, value, error = (summed(counts_to, counts_chip, k) for k in range(3))
    squares = summed(counts_to, counts_chip, 3, 8)
    mine = lane == sub + first

    def per_slot(x):
        return jnp.sum(x, axis=1, keepdims=True)

    innov_sum = per_slot(
        jnp.where(mine, jnp.sum(squares[0:3], axis=0, keepdims=True), 0.0)
        + mean * (count * mean - 2.0 * value)
    )
    error_error = per_slot(jnp.where(mine, jnp.sum(squares[3:6], axis=0, keepdims=True), 0.0))
    count_spread = count * spread
    spread_sum = per_slot(count_spread)
    spread_spread = per_slot(count_spread * spread)
    spread_error = per_slot(spread * error)
    error_sum = per_slot(error)
    weight_var = (
        2.0 * prior_mean * prior_mean * (1.0 + spread_spread)
        + 4.0 * prior_mean * spread_error
        + 2.0 * error_error
    )
    lam = jnp.maximum(
        (prior_mean * weight_var + prior_var * spread_sum * (innov_sum - error_sum))
        / (weight_var + prior_var * spread_sum * spread_sum),
        1.0,
    )
    placed = jnp.where(in_block, lam, 0.0)
    for r in range(32):
        to_region[r] = jnp.sum(
            jnp.where((ids_col >> 7) == r, placed, 0.0), axis=0, keepdims=True
        )
    my_lam[...] = jnp.sum(jnp.where(mine, lam, 0.0), axis=0, keepdims=True)

    def to_all(some):
        for i, (peer, dest) in some:
            pltpu.make_async_remote_copy(
                src_ref=to_region.at[peer],
                dst_ref=from_region.at[pl.ds(i, 1)],
                send_sem=reg_send,
                recv_sem=reg_recv,
                device_id={"region": peer, "member": dest},
                device_id_type=MESH,
            ).start()

    everyone = list(enumerate(peers))
    pl.semaphore_wait(all_sem, len(along_z))
    to_all(everyone[:96])
    lam_copies = []
    for i, peer in enumerate(others):
        lam_copies.append(
            pltpu.make_async_remote_copy(
                src_ref=my_lam,
                dst_ref=lams.at[i],
                send_sem=lam_send.at[i],
                recv_sem=lam_recv.at[i],
                device_id={"member": peer},
                device_id_type=MESH,
            )
        )
        lam_copies[-1].start()
    mean_copies = []
    for i, peer in enumerate(others):
        mean_copies.append(
            pltpu.make_async_remote_copy(
                src_ref=means.at[my_rows],
                dst_ref=means.at[my_rows],
                send_sem=mean_send.at[i],
                recv_sem=mean_recv.at[i],
                device_id={"member": peer},
                device_id_type=MESH,
            )
        )
        mean_copies[-1].start()

    to_all(everyone[96:])
    for copy in lam_copies:
        copy.wait_recv()
    lam_row = my_lam[...]
    for i in range(len(others)):
        lam_row = lam_row + lams[i]
    eye = lax.broadcasted_iota(I32, (LANES, LANES), 0) == lax.broadcasted_iota(
        I32, (LANES, LANES), 1
    )
    lam_col = jnp.sum(jnp.where(eye, lam_row, 0.0), axis=1, keepdims=True)
    scale[...] = jnp.broadcast_to(jnp.sqrt(lam_col), (LANES, LANES))
    for copy in mean_copies:
        copy.wait_recv()

    @pl.loop(0, 16)
    def _(j):
        for i in range(8):
            at = pl.ds(pl.multiple_of(j * 1024 + i * LANES, LANES), LANES)
            row = pl.ds(HALF * (i % 2) + 4 * j + i // 2, 1)
            m = means[row, :]
            x = ens_v[:, at].astype(F32)
            out[:, at] = (m + scale[row, :] * (x - m)).astype(BF16)

    arrived = pltpu.make_async_remote_copy(
        src_ref=from_region.at[0:255],
        dst_ref=from_region.at[0:255],
        send_sem=reg_send,
        recv_sem=reg_recv,
        device_id={"member": others[0]},
        device_id_type=MESH,
    )
    arrived.wait_recv()
    post_row = to_region[region] + jnp.sum(from_region[...], axis=0, keepdims=True)
    turned = pltpu.roll(jnp.broadcast_to(post_row, (8, LANES)), (8 - member) * OWN % LANES, 1)
    post[...] = turned[0:1, :OWN]

    for k in range(2):
        for d in order:
            core_copy(k, d).wait_send()
            if d:
                chip_copy(k, d).wait_send()
    for copy in (*mean_copies, *lam_copies, arrived):
        copy.wait_send()


def written(a, b, a_out, b_out, sem):
    copies = [
        pltpu.make_async_copy(a, a_out, sem.at[0]),
        pltpu.make_async_copy(b, b_out, sem.at[1]),
    ]
    for copy in copies:
        copy.start()
    for copy in copies:
        copy.wait()


def body(ensemble, obs_value, obs_var, obs_point, owned_blocks, infl_mean, infl_var):
    anywhere = pl.BlockSpec(memory_space=pl.ANY)
    vmem = pl.BlockSpec(memory_space=pltpu.VMEM)
    dma = pltpu.SemaphoreType.DMA
    inflated, post = pl.pallas_call(
        kernel,
        out_shape=(pltpu.VMEM(ensemble.shape, BF16), pltpu.VMEM((1, OWN), F32)),
        in_specs=[anywhere] * 7,
        out_specs=(vmem, vmem),
        scratch_shapes=[
            pltpu.VMEM((10, 16384), BF16),
            pltpu.VMEM((32, LANES), F32),
            pltpu.VMEM((32, LANES), F32),
            pltpu.VMEM((32, LANES), I32),
            pltpu.VMEM((1, LANES), I32),
            pltpu.VMEM((32, LANES), F32),
            pltpu.VMEM((32, LANES), F32),
            pltpu.VMEM((5 * HALF, 2 * LANES), F32),
            pltpu.VMEM((16, HALF), F32),
            *[
                pltpu.VMEM((*lead, rows, LANES), F32)
                for lead in ((2, 4), (4,), (4,), (3,))
                for rows in (POINTS, COUNTS)
            ],
            pltpu.VMEM((LANES, LANES), F32),
            pltpu.VMEM((1, LANES), F32),
            pltpu.VMEM((7, 1, LANES), F32),
            pltpu.VMEM((LANES, LANES), F32),
            pltpu.VMEM((32, 1, LANES), F32),
            pltpu.VMEM((256, LANES), F32),
            dma((7,)),
            pltpu.SemaphoreType.REGULAR,
            pltpu.SemaphoreType.REGULAR,
            *[dma((n,)) for n in (8, 6, 7, 7) for _ in range(2)],
            dma,
            dma,
        ],
        compiler_params=pltpu.CompilerParams(collective_id=0, has_side_effects=True),
    )(
        ensemble,
        obs_value,
        obs_var,
        obs_point,
        owned_blocks.reshape(1, -1),
        infl_mean.reshape(32, LANES),
        infl_var.reshape(32, LANES),
    )
    inflated, post = pl.pallas_call(
        written,
        out_shape=(
            jax.ShapeDtypeStruct(ensemble.shape, BF16),
            jax.ShapeDtypeStruct((1, OWN), F32),
        ),
        in_specs=(vmem, vmem),
        out_specs=(anywhere, anywhere),
        scratch_shapes=[dma((2,))],
    )(
        pltpu.with_memory_space_constraint(inflated, pltpu.VMEM),
        pltpu.with_memory_space_constraint(post, pltpu.VMEM),
    )
    return inflated, post.reshape(-1)


def solution(mesh):
    placed = (
        P("member", "region"),
        P(("region", "member"), None),
        P(("region", "member"), None),
        P(("region", "member"), None),
        P("region"),
        P(),
        P(),
    )
    return jax.shard_map(
        body,
        mesh=mesh,
        in_specs=placed,
        out_specs=(P("member", "region"), P(("region", "member"))),
        check_vma=False,
    )
```

```python
import jax
import jax.numpy as jnp
from jax import lax
from jax.experimental import pallas as pl
from jax.experimental.pallas import tpu as pltpu
from jax.sharding import PartitionSpec as P

MESH = pl.DeviceIdType.MESH
F32 = jnp.float32
BF16 = jnp.bfloat16
I32 = jnp.int32
OWN = 16
LANES = 128
HALF = 64
POINTS = 2 * OWN
COUNTS = 3 * OWN + 8
STEP = 32


def parts_of(x, count):
    parts = []
    for _ in range(count):
        parts.append(x.astype(BF16))
        x = x - parts[-1].astype(F32)
    return [p.astype(F32) for p in parts]


def point_sums(ens_v, sums):
    @pl.loop(0, 16)
    def _(j):
        x = ens_v[:, pl.ds(pl.multiple_of(j * 1024, 1024), 1024)].astype(F32)
        total = jnp.sum(x, axis=0, keepdims=True)
        square = jnp.sum(x * x, axis=0, keepdims=True)
        for i in range(8):
            row = 4 * (j % 4) + i // 2
            piece = sums.at[i % 2, j // 4]
            piece[pl.ds(row, 1), :] = total[:, i * LANES : (i + 1) * LANES]
            piece[pl.ds(OWN + row, 1), :] = square[:, i * LANES : (i + 1) * LANES]


def tall(row, rows):
    same = jnp.broadcast_to(row, (16, LANES)).astype(BF16)
    return jnp.concatenate([same] * (rows // 16), axis=0)


def histograms(val_v, var_v, pnt_v, rows_v, acc, acc_q, counts):
    across = (((1,), (1,)), ((), ()))
    point, value, var = pnt_v[...], val_v[...], var_v[...]
    odd = ((point >> 7) & 1).astype(F32)
    squares = [*parts_of(value * value, 2), *parts_of(var * var, 2)]
    kinds = [
        (point >> 8).astype(F32),
        (point & 255).astype(F32),
        *parts_of(value, 2),
        *parts_of(var, 2),
        *(p * (1.0 - odd) for p in squares),
        *(p * odd for p in squares),
    ]
    for k, kind in enumerate(kinds):
        rows_v[k] = kind
    index = lax.broadcasted_iota(I32, (256, LANES), 0).astype(F32).astype(BF16)
    none, one = jnp.zeros((256, LANES), BF16), jnp.ones((256, LANES), BF16)
    sub = lax.broadcasted_iota(I32, (8, LANES), 0)

    def step(first):
        left, right, square = [], [], []
        for i in range(STEP):
            row = [rows_v[k, pl.ds(first + i, 1), :] for k in range(14)]
            in_high = index[:HALF] == tall(row[0], HALF)
            in_low = index == tall(row[1], 256)
            left.append(
                jnp.concatenate(
                    [
                        jnp.where(in_high, one[:HALF], none[:HALF]),
                        *(jnp.where(in_high, tall(w, HALF), none[:HALF]) for w in row[2:6]),
                    ],
                    axis=0,
                )
            )
            right.append(jnp.where(in_low, one, none))
            stack = jnp.broadcast_to(row[6], (8, LANES))
            for k in range(1, 8):
                stack = jnp.where(sub == k, row[6 + k], stack)
            square.append(stack)
        left = jnp.concatenate(left, axis=1)
        right = jnp.concatenate(right, axis=1)
        square = jnp.concatenate(square, axis=1).astype(BF16)
        return (
            lax.dot_general(left, right, across, preferred_element_type=F32),
            lax.dot_general(square, left[:HALF], across, preferred_element_type=F32),
        )

    if STEP == 32:
        acc[...], acc_q[...] = step(0)
    else:
        acc[...], acc_q[...] = jnp.zeros_like(acc), jnp.zeros_like(acc_q)

        @pl.loop(0, 32 // STEP)
        def _(i):
            more, more_q = step(i * STEP)
            acc[...] += more
            acc_q[...] += more_q

    squares = jnp.concatenate([acc_q[:4, :], acc_q[4:, :]], axis=1)
    squares = jnp.concatenate([squares, squares], axis=0)
    for parity in range(2):
        lanes = slice(parity * LANES, (parity + 1) * LANES)
        for y in range(4):
            part = [
                acc[k * HALF + y * OWN : k * HALF + (y + 1) * OWN, lanes] for k in range(5)
            ]
            piece = counts.at[parity, y]
            piece[:OWN, :] = part[0]
            piece[OWN : 2 * OWN, :] = part[1] + part[2]
            piece[2 * OWN : 3 * OWN, :] = part[3] + part[4]
            piece[3 * OWN :, :] = squares


def looked_up(tables, ids_col):
    slots = ids_col.shape[0]
    lane = lax.broadcasted_iota(I32, (slots, LANES), 1)
    in_row = (lax.broadcasted_iota(I32, (slots, 32), 1) == (ids_col >> 7)).astype(F32)
    cols = []
    for table in tables:
        picked = jnp.dot(
            in_row, table[...], precision=lax.Precision.HIGHEST, preferred_element_type=F32
        )
        cols.append(
            jnp.sum(jnp.where(lane == (ids_col & 127), picked, 0.0), axis=1, keepdims=True)
        )
    return cols


def kernel(
    ens, val, var, pnt, own, mean_tab, var_tab,
    out, post,
    ens_v, val_v, var_v, pnt_v, own_v, mean_v, ivar_v,
    rows_v, acc, acc_q, sums, counts, sums_core, counts_core, sums_to, counts_to, sums_chip, counts_chip, means, my_lam, lams, scale, to_region, from_region,
    load_sem, line_sem, all_sem, core_send, core_recv, chip_send, chip_recv,
    mean_send, mean_recv, lam_send, lam_recv, reg_send, reg_recv,
):
    loads = [
        pltpu.make_async_copy(a, b, load_sem.at[i])
        for i, (a, b) in enumerate(
            (
                (pnt, pnt_v),
                (val, val_v),
                (var, var_v),
                (ens, ens_v),
                (own, own_v),
                (mean_tab, mean_v),
                (var_tab, ivar_v),
            )
        )
    ]
    for load in loads:
        load.start()
    from_region[255:256, :] = jnp.zeros((1, LANES), F32)

    region, member = lax.axis_index("region"), lax.axis_index("member")
    y, core = lax.div(member, 2), lax.rem(member, 2)
    ys = [y, *(lax.rem(y + d, 4) for d in range(1, 4))]
    others = [2 * ys[d] + c for d in (2, 1, 3) for c in (core, 1 - core)] + [2 * y + 1 - core]
    x, z = lax.div(region, 8), lax.rem(region, 8)
    xs = [8 * lax.rem(x + d, 4) for d in range(4)]
    zs = [lax.rem(z + d, 8) for d in range(8)]
    along_x = [xs[d] + zs[0] for d in (2, 1, 3)]
    along_z = [xs[0] + zs[d] for d in (4, 3, 5, 2, 6, 1, 7)]
    members = [2 * ys[d] + c for d in range(4) for c in (core, 1 - core)]
    apart = sorted(
        (
            (-sum(min(a, n - a) for a, n in zip(d[:3], (4, 8, 4))), d)
            for d in ((dx, dz, dy, c) for dx in range(4) for dz in range(8) for dy in range(4) for c in range(2))
            if any(d)
        )
    )
    peers = [(xs[dx] + zs[dz], members[2 * dy + c]) for _, (dx, dz, dy, c) in apart]

    barrier = pltpu.get_barrier_semaphore()
    for peer in (along_x[0], *along_z[3:5]):
        pl.semaphore_signal(barrier, inc=1, device_id={"region": peer}, device_id_type=MESH)
    for peer in others:
        pl.semaphore_signal(barrier, inc=1, device_id={"member": peer}, device_id_type=MESH)
    for peer in (*along_x[1:], *along_z[5:]):
        pl.semaphore_signal(barrier, inc=1, device_id={"region": peer}, device_id_type=MESH)

    for load in loads[:3]:
        load.wait()
    histograms(val_v, var_v, pnt_v, rows_v, acc, acc_q, counts)

    pl.semaphore_wait(barrier, len(others) + len(along_x) + 4)

    order = (1, 3, 0)
    def core_copy(k, d):
        return pltpu.make_async_remote_copy(
            src_ref=(sums, counts)[k].at[1 - core, ys[d]],
            dst_ref=(sums_core, counts_core)[k].at[d],
            send_sem=core_send.at[4 * k + d],
            recv_sem=core_recv.at[4 * k + d],
            device_id={"member": 2 * y + 1 - core},
            device_id_type=MESH,
        )

    def chip_copy(k, d, turn=0):
        i = 3 if turn else d - 1
        to = 1 - core if turn else core
        return pltpu.make_async_remote_copy(
            src_ref=(sums, counts)[k].at[to, ys[2]] if d == 2 else (sums_to, counts_to)[k].at[d],
            dst_ref=(sums_chip, counts_chip)[k].at[i],
            send_sem=chip_send.at[4 * k + i],
            recv_sem=chip_recv.at[4 * k + i],
            device_id={"member": 2 * ys[d] + to},
            device_id_type=MESH,
        )

    chip_copies = [(k, d, turn) for k in (1, 0) for d, turn in ((1, 0), (3, 0), (2, 0), (2, 1))]

    def pass_on(k):
        own, came, total = ((sums, sums_core, sums_to), (counts, counts_core, counts_to))[k]
        for d in order:
            core_copy(k, d).wait_recv()
            total[d] = own[core, ys[d]] + came[d]
            if d:
                chip_copy(k, d).start()

    for d in order:
        core_copy(1, d).start()
    for turn in range(2):
        chip_copy(1, 2, turn).start()
    for peer in (*along_x, *along_z[3:5]):
        pl.semaphore_signal(line_sem, inc=1, device_id={"region": peer}, device_id_type=MESH)
    for load in loads[3:]:
        load.wait()
    point_sums(ens_v, sums)
    for d in order:
        core_copy(0, d).start()
    for turn in range(2):
        chip_copy(0, 2, turn).start()
    pass_on(1)
    pass_on(0)
    pl.semaphore_wait(line_sem, len(along_x) + 2)
    for peer in along_z:
        pl.semaphore_signal(all_sem, inc=1, device_id={"region": peer}, device_id_type=MESH)

    sub = lax.broadcasted_iota(I32, (OWN, LANES), 0)
    lane = lax.broadcasted_iota(I32, (OWN, LANES), 1)
    ids_col = jnp.sum(
        jnp.where(lane == 2 * (OWN * y + sub) + core, own_v[...].astype(F32), 0.0),
        axis=1,
        keepdims=True,
    ).astype(I32)
    prior_mean, prior_var = looked_up((mean_v, ivar_v), ids_col)
    in_block = lane == (ids_col & 127)

    for copy in chip_copies:
        chip_copy(*copy).wait_recv()

    def summed(total, came, k, size=OWN):
        at = slice(k * OWN, k * OWN + size)
        near = total[0, at, :] + (came[0, at, :] + came[2, at, :])
        return near + (came[1, at, :] + came[3, at, :])

    mean = summed(sums_to, sums_chip, 0) / 80.0
    first = core * HALF + y * OWN
    my_rows = pl.ds(pl.multiple_of(first, OWN), OWN)
    means[my_rows, :] = mean
    spread = (summed(sums_to, sums_chip, 1) - 80.0 * mean * mean) / 79.0
    count, value, error = (summed(counts_to, counts_chip, k) for k in range(3))
    squares = summed(counts_to, counts_chip, 3, 8)
    mine = lane == sub + first

    def per_slot(x):
        return jnp.sum(x, axis=1, keepdims=True)

    innov_sum = per_slot(
        jnp.where(mine, jnp.sum(squares[0:2], axis=0, keepdims=True), 0.0)
        + mean * (count * mean - 2.0 * value)
    )
    error_error = per_slot(jnp.where(mine, jnp.sum(squares[2:4], axis=0, keepdims=True), 0.0))
    count_spread = count * spread
    spread_sum = per_slot(count_spread)
    spread_spread = per_slot(count_spread * spread)
    spread_error = per_slot(spread * error)
    error_sum = per_slot(error)
    weight_var = (
        2.0 * prior_mean * prior_mean * (1.0 + spread_spread)
        + 4.0 * prior_mean * spread_error
        + 2.0 * error_error
    )
    lam = jnp.maximum(
        (prior_mean * weight_var + prior_var * spread_sum * (innov_sum - error_sum))
        / (weight_var + prior_var * spread_sum * spread_sum),
        1.0,
    )
    placed = jnp.where(in_block, lam, 0.0)
    for r in range(32):
        to_region[r] = jnp.sum(
            jnp.where((ids_col >> 7) == r, placed, 0.0), axis=0, keepdims=True
        )
    my_lam[...] = jnp.sum(jnp.where(mine, lam, 0.0), axis=0, keepdims=True)

    def to_all(some):
        for i, (peer, dest) in some:
            pltpu.make_async_remote_copy(
                src_ref=to_region.at[peer],
                dst_ref=from_region.at[pl.ds(i, 1)],
                send_sem=reg_send,
                recv_sem=reg_recv,
                device_id={"region": peer, "member": dest},
                device_id_type=MESH,
            ).start()

    everyone = list(enumerate(peers))
    pl.semaphore_wait(all_sem, len(along_z))
    to_all(everyone[:96])
    lam_copies = []
    for i, peer in enumerate(others):
        lam_copies.append(
            pltpu.make_async_remote_copy(
                src_ref=my_lam,
                dst_ref=lams.at[i],
                send_sem=lam_send.at[i],
                recv_sem=lam_recv.at[i],
                device_id={"member": peer},
                device_id_type=MESH,
            )
        )
        lam_copies[-1].start()
    mean_copies = []
    for i, peer in enumerate(others):
        mean_copies.append(
            pltpu.make_async_remote_copy(
                src_ref=means.at[my_rows],
                dst_ref=means.at[my_rows],
                send_sem=mean_send.at[i],
                recv_sem=mean_recv.at[i],
                device_id={"member": peer},
                device_id_type=MESH,
            )
        )
        mean_copies[-1].start()

    to_all(everyone[96:])
    for copy in lam_copies:
        copy.wait_recv()
    lam_row = my_lam[...]
    for i in range(len(others)):
        lam_row = lam_row + lams[i]
    eye = lax.broadcasted_iota(I32, (LANES, LANES), 0) == lax.broadcasted_iota(
        I32, (LANES, LANES), 1
    )
    lam_col = jnp.sum(jnp.where(eye, lam_row, 0.0), axis=1, keepdims=True)
    scale[...] = jnp.broadcast_to(jnp.sqrt(lam_col), (LANES, LANES))
    for copy in mean_copies:
        copy.wait_recv()

    @pl.loop(0, 16)
    def _(j):
        for i in range(8):
            at = pl.ds(pl.multiple_of(j * 1024 + i * LANES, LANES), LANES)
            row = pl.ds(HALF * (i % 2) + 4 * j + i // 2, 1)
            m = means[row, :]
            x = ens_v[:, at].astype(F32)
            out[:, at] = (m + scale[row, :] * (x - m)).astype(BF16)

    arrived = pltpu.make_async_remote_copy(
        src_ref=from_region.at[0:255],
        dst_ref=from_region.at[0:255],
        send_sem=reg_send,
        recv_sem=reg_recv,
        device_id={"member": others[0]},
        device_id_type=MESH,
    )
    for k in range(2):
        for d in order:
            core_copy(k, d).wait_send()
    for copy in chip_copies:
        chip_copy(*copy).wait_send()
    for copy in (*mean_copies, *lam_copies, arrived):
        copy.wait_send()
    arrived.wait_recv()
    post_row = to_region[region] + jnp.sum(from_region[...], axis=0, keepdims=True)
    turned = pltpu.roll(jnp.broadcast_to(post_row, (8, LANES)), (8 - member) * OWN % LANES, 1)
    post[...] = turned[0:1, :OWN]


def written(a, b, a_out, b_out, sem):
    copies = [
        pltpu.make_async_copy(a, a_out, sem.at[0]),
        pltpu.make_async_copy(b, b_out, sem.at[1]),
    ]
    for copy in copies:
        copy.start()
    for copy in copies:
        copy.wait()


def body(ensemble, obs_value, obs_var, obs_point, owned_blocks, infl_mean, infl_var):
    anywhere = pl.BlockSpec(memory_space=pl.ANY)
    vmem = pl.BlockSpec(memory_space=pltpu.VMEM)
    dma = pltpu.SemaphoreType.DMA
    inflated, post = pl.pallas_call(
        kernel,
        out_shape=(pltpu.VMEM(ensemble.shape, BF16), pltpu.VMEM((1, OWN), F32)),
        in_specs=[anywhere] * 7,
        out_specs=(vmem, vmem),
        scratch_shapes=[
            pltpu.VMEM((10, 16384), BF16),
            pltpu.VMEM((32, LANES), F32),
            pltpu.VMEM((32, LANES), F32),
            pltpu.VMEM((32, LANES), I32),
            pltpu.VMEM((1, LANES), I32),
            pltpu.VMEM((32, LANES), F32),
            pltpu.VMEM((32, LANES), F32),
            pltpu.VMEM((14, 32, LANES), F32),
            pltpu.VMEM((5 * HALF, 2 * LANES), F32),
            pltpu.VMEM((8, HALF), F32),
            *[
                pltpu.VMEM((*lead, rows, LANES), F32)
                for lead in ((2, 4), (4,), (4,), (4,))
                for rows in (POINTS, COUNTS)
            ],
            pltpu.VMEM((LANES, LANES), F32),
            pltpu.VMEM((1, LANES), F32),
            pltpu.VMEM((7, 1, LANES), F32),
            pltpu.VMEM((LANES, LANES), F32),
            pltpu.VMEM((32, 1, LANES), F32),
            pltpu.VMEM((256, LANES), F32),
            dma((7,)),
            pltpu.SemaphoreType.REGULAR,
            pltpu.SemaphoreType.REGULAR,
            *[dma((n,)) for n in (8, 8, 7, 7) for _ in range(2)],
            dma,
            dma,
        ],
        compiler_params=pltpu.CompilerParams(collective_id=0, has_side_effects=True),
    )(
        ensemble,
        obs_value,
        obs_var,
        obs_point,
        owned_blocks.reshape(1, -1),
        infl_mean.reshape(32, LANES),
        infl_var.reshape(32, LANES),
    )
    inflated, post = pl.pallas_call(
        written,
        out_shape=(
            jax.ShapeDtypeStruct(ensemble.shape, BF16),
            jax.ShapeDtypeStruct((1, OWN), F32),
        ),
        in_specs=(vmem, vmem),
        out_specs=(anywhere, anywhere),
        scratch_shapes=[dma((2,))],
    )(
        pltpu.with_memory_space_constraint(inflated, pltpu.VMEM),
        pltpu.with_memory_space_constraint(post, pltpu.VMEM),
    )
    return inflated, post.reshape(-1)


def solution(mesh):
    placed = (
        P("member", "region"),
        P(("region", "member"), None),
        P(("region", "member"), None),
        P(("region", "member"), None),
        P("region"),
        P(),
        P(),
    )
    return jax.shard_map(
        body,
        mesh=mesh,
        in_specs=placed,
        out_specs=(P("member", "region"), P(("region", "member"))),
        check_vma=False,
    )
```

```python
import jax
import jax.numpy as jnp
from jax import lax
from jax.experimental import pallas as pl
from jax.experimental.pallas import tpu as pltpu
from jax.sharding import PartitionSpec as P

MESH = pl.DeviceIdType.MESH
F32 = jnp.float32
BF16 = jnp.bfloat16
I32 = jnp.int32
OWN = 16
LANES = 128
HALF = 64
POINTS = 2 * OWN
COUNTS = 3 * OWN + 8
STEP = 32


def parts_of(x, count):
    parts = []
    for _ in range(count):
        parts.append(x.astype(BF16))
        x = x - parts[-1].astype(F32)
    return [p.astype(F32) for p in parts]


def point_sums(ens_v, sums):
    @pl.loop(0, 16)
    def _(j):
        x = ens_v[:, pl.ds(pl.multiple_of(j * 1024, 1024), 1024)].astype(F32)
        total = jnp.sum(x, axis=0, keepdims=True)
        square = jnp.sum(x * x, axis=0, keepdims=True)
        for i in range(8):
            row = 4 * (j % 4) + i // 2
            piece = sums.at[i % 2, j // 4]
            piece[pl.ds(row, 1), :] = total[:, i * LANES : (i + 1) * LANES]
            piece[pl.ds(OWN + row, 1), :] = square[:, i * LANES : (i + 1) * LANES]


def tall(row, rows):
    same = jnp.broadcast_to(row, (16, LANES)).astype(BF16)
    return jnp.concatenate([same] * (rows // 16), axis=0)


def histograms(val_v, var_v, pnt_v, rows_v, acc, acc_q, counts):
    across = (((1,), (1,)), ((), ()))
    point, value, var = pnt_v[...], val_v[...], var_v[...]
    odd = ((point >> 7) & 1).astype(F32)
    squares = [*parts_of(value * value, 2), *parts_of(var * var, 2)]
    kinds = [
        (point >> 8).astype(F32),
        (point & 255).astype(F32),
        *parts_of(value, 2),
        *parts_of(var, 2),
        *(p * (1.0 - odd) for p in squares),
        *(p * odd for p in squares),
    ]
    for k, kind in enumerate(kinds):
        rows_v[k] = kind
    index = lax.broadcasted_iota(I32, (256, LANES), 0).astype(F32).astype(BF16)
    none, one = jnp.zeros((256, LANES), BF16), jnp.ones((256, LANES), BF16)
    sub = lax.broadcasted_iota(I32, (8, LANES), 0)

    def step(first):
        left, right, square = [], [], []
        for i in range(STEP):
            row = [rows_v[k, pl.ds(first + i, 1), :] for k in range(14)]
            in_high = index[:HALF] == tall(row[0], HALF)
            in_low = index == tall(row[1], 256)
            left.append(
                jnp.concatenate(
                    [
                        jnp.where(in_high, one[:HALF], none[:HALF]),
                        *(jnp.where(in_high, tall(w, HALF), none[:HALF]) for w in row[2:6]),
                    ],
                    axis=0,
                )
            )
            right.append(jnp.where(in_low, one, none))
            stack = jnp.broadcast_to(row[6], (8, LANES))
            for k in range(1, 8):
                stack = jnp.where(sub == k, row[6 + k], stack)
            square.append(stack)
        left = jnp.concatenate(left, axis=1)
        right = jnp.concatenate(right, axis=1)
        square = jnp.concatenate(square, axis=1).astype(BF16)
        return (
            lax.dot_general(left, right, across, preferred_element_type=F32),
            lax.dot_general(square, left[:HALF], across, preferred_element_type=F32),
        )

    if STEP == 32:
        acc[...], acc_q[...] = step(0)
    else:
        acc[...], acc_q[...] = jnp.zeros_like(acc), jnp.zeros_like(acc_q)

        @pl.loop(0, 32 // STEP)
        def _(i):
            more, more_q = step(i * STEP)
            acc[...] += more
            acc_q[...] += more_q

    squares = jnp.concatenate([acc_q[:4, :], acc_q[4:, :]], axis=1)
    squares = jnp.concatenate([squares, squares], axis=0)
    for parity in range(2):
        lanes = slice(parity * LANES, (parity + 1) * LANES)
        for y in range(4):
            part = [
                acc[k * HALF + y * OWN : k * HALF + (y + 1) * OWN, lanes] for k in range(5)
            ]
            piece = counts.at[parity, y]
            piece[:OWN, :] = part[0]
            piece[OWN : 2 * OWN, :] = part[1] + part[2]
            piece[2 * OWN : 3 * OWN, :] = part[3] + part[4]
            piece[3 * OWN :, :] = squares


def looked_up(tables, ids_col):
    slots = ids_col.shape[0]
    lane = lax.broadcasted_iota(I32, (slots, LANES), 1)
    in_row = (lax.broadcasted_iota(I32, (slots, 32), 1) == (ids_col >> 7)).astype(F32)
    cols = []
    for table in tables:
        picked = jnp.dot(
            in_row, table[...], precision=lax.Precision.HIGHEST, preferred_element_type=F32
        )
        cols.append(
            jnp.sum(jnp.where(lane == (ids_col & 127), picked, 0.0), axis=1, keepdims=True)
        )
    return cols


def kernel(
    ens, val, var, pnt, own, mean_tab, var_tab,
    out, post,
    ens_v, val_v, var_v, pnt_v, own_v, mean_v, ivar_v,
    rows_v, acc, acc_q, sums, counts, sums_core, counts_core, sums_to, counts_to, sums_chip, counts_chip, means, my_lam, lams, scale, to_region, from_region,
    load_sem, line_sem, all_sem, core_send, core_recv, chip_send, chip_recv,
    mean_send, mean_recv, lam_send, lam_recv, reg_send, reg_recv,
):
    loads = [
        pltpu.make_async_copy(a, b, load_sem.at[i])
        for i, (a, b) in enumerate(
            (
                (pnt, pnt_v),
                (val, val_v),
                (var, var_v),
                (ens, ens_v),
                (own, own_v),
                (mean_tab, mean_v),
                (var_tab, ivar_v),
            )
        )
    ]
    for load in loads:
        load.start()
    from_region[255:256, :] = jnp.zeros((1, LANES), F32)

    region, member = lax.axis_index("region"), lax.axis_index("member")
    y, core = lax.div(member, 2), lax.rem(member, 2)
    ys = [y, *(lax.rem(y + d, 4) for d in range(1, 4))]
    others = [2 * ys[d] + c for d in (2, 1, 3) for c in (core, 1 - core)] + [2 * y + 1 - core]
    x, z = lax.div(region, 8), lax.rem(region, 8)
    xs = [8 * lax.rem(x + d, 4) for d in range(4)]
    zs = [lax.rem(z + d, 8) for d in range(8)]
    along_x = [xs[d] + zs[0] for d in (2, 1, 3)]
    along_z = [xs[0] + zs[d] for d in (4, 3, 5, 2, 6, 1, 7)]
    members = [2 * ys[d] + c for d in range(4) for c in (core, 1 - core)]
    apart = sorted(
        (
            (-sum(min(a, n - a) for a, n in zip(d[:3], (4, 8, 4))), d)
            for d in ((dx, dz, dy, c) for dx in range(4) for dz in range(8) for dy in range(4) for c in range(2))
            if any(d)
        )
    )
    peers = [(xs[dx] + zs[dz], members[2 * dy + c]) for _, (dx, dz, dy, c) in apart]

    barrier = pltpu.get_barrier_semaphore()
    for peer in (along_x[0], *along_z[3:5]):
        pl.semaphore_signal(barrier, inc=1, device_id={"region": peer}, device_id_type=MESH)
    for peer in others:
        pl.semaphore_signal(barrier, inc=1, device_id={"member": peer}, device_id_type=MESH)
    for peer in (*along_x[1:], *along_z[5:]):
        pl.semaphore_signal(barrier, inc=1, device_id={"region": peer}, device_id_type=MESH)

    for load in loads[:3]:
        load.wait()
    histograms(val_v, var_v, pnt_v, rows_v, acc, acc_q, counts)

    pl.semaphore_wait(barrier, len(others) + len(along_x) + 4)

    def core_copy(k, d):
        return pltpu.make_async_remote_copy(
            src_ref=(sums, counts)[k].at[1 - core, ys[d]],
            dst_ref=(sums_core, counts_core)[k].at[d],
            send_sem=core_send.at[4 * k + d],
            recv_sem=core_recv.at[4 * k + d],
            device_id={"member": 2 * y + 1 - core},
            device_id_type=MESH,
        )

    def chip_copy(k, d, turn=0):
        i = 3 if turn else d - 1
        to = 1 - core if turn else core
        direct = k == 1 and d == 2
        return pltpu.make_async_remote_copy(
            src_ref=counts.at[to, ys[2]] if direct else (sums_to, counts_to)[k].at[d],
            dst_ref=(sums_chip, counts_chip)[k].at[i],
            send_sem=chip_send.at[4 * k + i],
            recv_sem=chip_recv.at[4 * k + i],
            device_id={"member": 2 * ys[d] + to},
            device_id_type=MESH,
        )

    chip_copies = [(1, 1, 0), (1, 3, 0), (0, 1, 0), (0, 3, 0), (1, 2, 0), (1, 2, 1), (0, 2, 0)]
    core_copies = [(1, 1), (1, 3), (0, 2), (0, 1), (0, 3), (1, 0), (0, 0)]

    for turn in range(2):
        chip_copy(1, 2, turn).start()
    for copy in core_copies:
        if copy[0]:
            core_copy(*copy).start()
    for peer in (*along_x, *along_z[3:5]):
        pl.semaphore_signal(line_sem, inc=1, device_id={"region": peer}, device_id_type=MESH)
    for load in loads[3:]:
        load.wait()
    point_sums(ens_v, sums)
    for copy in core_copies:
        if not copy[0]:
            core_copy(*copy).start()
    for k, d in core_copies:
        own, came, total = ((sums, sums_core, sums_to), (counts, counts_core, counts_to))[k]
        core_copy(k, d).wait_recv()
        total[d] = own[core, ys[d]] + came[d]
        if d:
            chip_copy(k, d).start()
    pl.semaphore_wait(line_sem, len(along_x) + 2)
    for peer in along_z:
        pl.semaphore_signal(all_sem, inc=1, device_id={"region": peer}, device_id_type=MESH)

    sub = lax.broadcasted_iota(I32, (OWN, LANES), 0)
    lane = lax.broadcasted_iota(I32, (OWN, LANES), 1)
    ids_col = jnp.sum(
        jnp.where(lane == 2 * (OWN * y + sub) + core, own_v[...].astype(F32), 0.0),
        axis=1,
        keepdims=True,
    ).astype(I32)
    prior_mean, prior_var = looked_up((mean_v, ivar_v), ids_col)
    in_block = lane == (ids_col & 127)

    for copy in chip_copies:
        chip_copy(*copy).wait_recv()

    def summed(total, came, k, size=OWN):
        at = slice(k * OWN, k * OWN + size)
        terms = [came[i, at, :] for i in range(came.shape[0])]
        return total[0, at, :] + sum(terms[1:], terms[0])

    mean = summed(sums_to, sums_chip, 0) / 80.0
    first = core * HALF + y * OWN
    my_rows = pl.ds(pl.multiple_of(first, OWN), OWN)
    means[my_rows, :] = mean
    spread = (summed(sums_to, sums_chip, 1) - 80.0 * mean * mean) / 79.0
    count, value, error = (summed(counts_to, counts_chip, k) for k in range(3))
    squares = summed(counts_to, counts_chip, 3, 8)
    mine = lane == sub + first

    def per_slot(x):
        return jnp.sum(x, axis=1, keepdims=True)

    innov_sum = per_slot(
        jnp.where(mine, jnp.sum(squares[0:2], axis=0, keepdims=True), 0.0)
        + mean * (count * mean - 2.0 * value)
    )
    error_error = per_slot(jnp.where(mine, jnp.sum(squares[2:4], axis=0, keepdims=True), 0.0))
    count_spread = count * spread
    spread_sum = per_slot(count_spread)
    spread_spread = per_slot(count_spread * spread)
    spread_error = per_slot(spread * error)
    error_sum = per_slot(error)
    weight_var = (
        2.0 * prior_mean * prior_mean * (1.0 + spread_spread)
        + 4.0 * prior_mean * spread_error
        + 2.0 * error_error
    )
    lam = jnp.maximum(
        (prior_mean * weight_var + prior_var * spread_sum * (innov_sum - error_sum))
        / (weight_var + prior_var * spread_sum * spread_sum),
        1.0,
    )
    placed = jnp.where(in_block, lam, 0.0)
    for r in range(32):
        to_region[r] = jnp.sum(
            jnp.where((ids_col >> 7) == r, placed, 0.0), axis=0, keepdims=True
        )
    my_lam[...] = jnp.sum(jnp.where(mine, lam, 0.0), axis=0, keepdims=True)

    def to_all(some):
        for i, (peer, dest) in some:
            pltpu.make_async_remote_copy(
                src_ref=to_region.at[peer],
                dst_ref=from_region.at[pl.ds(i, 1)],
                send_sem=reg_send,
                recv_sem=reg_recv,
                device_id={"region": peer, "member": dest},
                device_id_type=MESH,
            ).start()

    everyone = list(enumerate(peers))
    pl.semaphore_wait(all_sem, len(along_z))
    to_all(everyone[:96])
    lam_copies = []
    for i, peer in enumerate(others):
        lam_copies.append(
            pltpu.make_async_remote_copy(
                src_ref=my_lam,
                dst_ref=lams.at[i],
                send_sem=lam_send.at[i],
                recv_sem=lam_recv.at[i],
                device_id={"member": peer},
                device_id_type=MESH,
            )
        )
        lam_copies[-1].start()
    mean_copies = []
    for i, peer in enumerate(others):
        mean_copies.append(
            pltpu.make_async_remote_copy(
                src_ref=means.at[my_rows],
                dst_ref=means.at[my_rows],
                send_sem=mean_send.at[i],
                recv_sem=mean_recv.at[i],
                device_id={"member": peer},
                device_id_type=MESH,
            )
        )
        mean_copies[-1].start()

    to_all(everyone[96:])
    for copy in lam_copies:
        copy.wait_recv()
    lam_row = my_lam[...]
    for i in range(len(others)):
        lam_row = lam_row + lams[i]
    eye = lax.broadcasted_iota(I32, (LANES, LANES), 0) == lax.broadcasted_iota(
        I32, (LANES, LANES), 1
    )
    lam_col = jnp.sum(jnp.where(eye, lam_row, 0.0), axis=1, keepdims=True)
    scale[...] = jnp.broadcast_to(jnp.sqrt(lam_col), (LANES, LANES))
    for copy in mean_copies:
        copy.wait_recv()

    @pl.loop(0, 16)
    def _(j):
        for i in range(8):
            at = pl.ds(pl.multiple_of(j * 1024 + i * LANES, LANES), LANES)
            row = pl.ds(HALF * (i % 2) + 4 * j + i // 2, 1)
            m = means[row, :]
            x = ens_v[:, at].astype(F32)
            out[:, at] = (m + scale[row, :] * (x - m)).astype(BF16)

    arrived = pltpu.make_async_remote_copy(
        src_ref=from_region.at[0:255],
        dst_ref=from_region.at[0:255],
        send_sem=reg_send,
        recv_sem=reg_recv,
        device_id={"member": others[0]},
        device_id_type=MESH,
    )
    for copy in core_copies:
        core_copy(*copy).wait_send()
    for copy in chip_copies:
        chip_copy(*copy).wait_send()
    for copy in (*mean_copies, *lam_copies, arrived):
        copy.wait_send()
    arrived.wait_recv()
    post_row = to_region[region] + jnp.sum(from_region[...], axis=0, keepdims=True)
    turned = pltpu.roll(jnp.broadcast_to(post_row, (8, LANES)), (8 - member) * OWN % LANES, 1)
    post[...] = turned[0:1, :OWN]


def written(a, b, a_out, b_out, sem):
    copies = [
        pltpu.make_async_copy(a, a_out, sem.at[0]),
        pltpu.make_async_copy(b, b_out, sem.at[1]),
    ]
    for copy in copies:
        copy.start()
    for copy in copies:
        copy.wait()


def body(ensemble, obs_value, obs_var, obs_point, owned_blocks, infl_mean, infl_var):
    anywhere = pl.BlockSpec(memory_space=pl.ANY)
    vmem = pl.BlockSpec(memory_space=pltpu.VMEM)
    dma = pltpu.SemaphoreType.DMA
    inflated, post = pl.pallas_call(
        kernel,
        out_shape=(pltpu.VMEM(ensemble.shape, BF16), pltpu.VMEM((1, OWN), F32)),
        in_specs=[anywhere] * 7,
        out_specs=(vmem, vmem),
        scratch_shapes=[
            pltpu.VMEM((10, 16384), BF16),
            pltpu.VMEM((32, LANES), F32),
            pltpu.VMEM((32, LANES), F32),
            pltpu.VMEM((32, LANES), I32),
            pltpu.VMEM((1, LANES), I32),
            pltpu.VMEM((32, LANES), F32),
            pltpu.VMEM((32, LANES), F32),
            pltpu.VMEM((14, 32, LANES), F32),
            pltpu.VMEM((5 * HALF, 2 * LANES), F32),
            pltpu.VMEM((8, HALF), F32),
            *[
                pltpu.VMEM((*lead, rows, LANES), F32)
                for lead in ((2, 4), (4,), (4,))
                for rows in (POINTS, COUNTS)
            ],
            pltpu.VMEM((3, POINTS, LANES), F32),
            pltpu.VMEM((4, COUNTS, LANES), F32),
            pltpu.VMEM((LANES, LANES), F32),
            pltpu.VMEM((1, LANES), F32),
            pltpu.VMEM((7, 1, LANES), F32),
            pltpu.VMEM((LANES, LANES), F32),
            pltpu.VMEM((32, 1, LANES), F32),
            pltpu.VMEM((256, LANES), F32),
            dma((7,)),
            pltpu.SemaphoreType.REGULAR,
            pltpu.SemaphoreType.REGULAR,
            *[dma((n,)) for n in (8, 8, 7, 7) for _ in range(2)],
            dma,
            dma,
        ],
        compiler_params=pltpu.CompilerParams(collective_id=0, has_side_effects=True),
    )(
        ensemble,
        obs_value,
        obs_var,
        obs_point,
        owned_blocks.reshape(1, -1),
        infl_mean.reshape(32, LANES),
        infl_var.reshape(32, LANES),
    )
    inflated, post = pl.pallas_call(
        written,
        out_shape=(
            jax.ShapeDtypeStruct(ensemble.shape, BF16),
            jax.ShapeDtypeStruct((1, OWN), F32),
        ),
        in_specs=(vmem, vmem),
        out_specs=(anywhere, anywhere),
        scratch_shapes=[dma((2,))],
    )(
        pltpu.with_memory_space_constraint(inflated, pltpu.VMEM),
        pltpu.with_memory_space_constraint(post, pltpu.VMEM),
    )
    return inflated, post.reshape(-1)


def solution(mesh):
    placed = (
        P("member", "region"),
        P(("region", "member"), None),
        P(("region", "member"), None),
        P(("region", "member"), None),
        P("region"),
        P(),
        P(),
    )
    return jax.shard_map(
        body,
        mesh=mesh,
        in_specs=placed,
        out_specs=(P("member", "region"), P(("region", "member"))),
        check_vma=False,
    )
```

```python
import jax
import jax.numpy as jnp
from jax import lax
from jax.experimental import pallas as pl
from jax.experimental.pallas import tpu as pltpu
from jax.sharding import PartitionSpec as P

MESH = pl.DeviceIdType.MESH
F32 = jnp.float32
BF16 = jnp.bfloat16
I32 = jnp.int32
OWN = 16
LANES = 128
HALF = 64
POINTS = 2 * OWN
COUNTS = 3 * OWN + 2
EARLY = 4
STEP = 32


def parts_of(x, count):
    parts = []
    for _ in range(count):
        parts.append(x.astype(BF16))
        x = x - parts[-1].astype(F32)
    return [p.astype(F32) for p in parts]


def point_sums(ens_v, sums, first, last):
    @pl.loop(first, last)
    def _(j):
        x = ens_v[:, pl.ds(pl.multiple_of(j * 1024, 1024), 1024)].astype(F32)
        total = jnp.sum(x, axis=0, keepdims=True)
        square = jnp.sum(x * x, axis=0, keepdims=True)
        for i in range(8):
            row = 4 * (j % 4) + i // 2
            piece = sums.at[i % 2, j // 4]
            piece[pl.ds(row, 1), :] = total[:, i * LANES : (i + 1) * LANES]
            piece[pl.ds(OWN + row, 1), :] = square[:, i * LANES : (i + 1) * LANES]


def tall(row, rows):
    same = jnp.broadcast_to(row, (16, LANES)).astype(BF16)
    return jnp.concatenate([same] * (rows // 16), axis=0)


def histograms(val_v, var_v, pnt_v, rows_v, acc, acc_q, counts):
    across = (((1,), (1,)), ((), ()))
    point, value, var = pnt_v[...], val_v[...], var_v[...]
    odd = ((point >> 7) & 1).astype(F32)
    squares = [*parts_of(value * value, 2), *parts_of(var * var, 2)]
    kinds = [
        (point >> 8).astype(F32),
        (point & 255).astype(F32),
        *parts_of(value, 2),
        *parts_of(var, 2),
        *(p * (1.0 - odd) for p in squares),
        *(p * odd for p in squares),
    ]
    for k, kind in enumerate(kinds):
        rows_v[k] = kind
    index = lax.broadcasted_iota(I32, (256, LANES), 0).astype(F32).astype(BF16)
    none, one = jnp.zeros((256, LANES), BF16), jnp.ones((256, LANES), BF16)
    sub = lax.broadcasted_iota(I32, (8, LANES), 0)

    def step(first):
        left, right, square = [], [], []
        for i in range(STEP):
            row = [rows_v[k, pl.ds(first + i, 1), :] for k in range(14)]
            in_high = index[:HALF] == tall(row[0], HALF)
            in_low = index == tall(row[1], 256)
            left.append(
                jnp.concatenate(
                    [
                        jnp.where(in_high, one[:HALF], none[:HALF]),
                        *(jnp.where(in_high, tall(w, HALF), none[:HALF]) for w in row[2:6]),
                    ],
                    axis=0,
                )
            )
            right.append(jnp.where(in_low, one, none))
            stack = jnp.broadcast_to(row[6], (8, LANES))
            for k in range(1, 8):
                stack = jnp.where(sub == k, row[6 + k], stack)
            square.append(stack)
        left = jnp.concatenate(left, axis=1)
        right = jnp.concatenate(right, axis=1)
        square = jnp.concatenate(square, axis=1).astype(BF16)
        return (
            lax.dot_general(left, right, across, preferred_element_type=F32),
            lax.dot_general(square, left[:HALF], across, preferred_element_type=F32),
        )

    if STEP == 32:
        acc[...], acc_q[...] = step(0)
    else:
        acc[...], acc_q[...] = jnp.zeros_like(acc), jnp.zeros_like(acc_q)

        @pl.loop(0, 32 // STEP)
        def _(i):
            more, more_q = step(i * STEP)
            acc[...] += more
            acc_q[...] += more_q

    squares = jnp.concatenate(
        [
            jnp.concatenate([acc_q[k : k + 1, :] + acc_q[k + 1 : k + 2, :] for k in (0, 2)], axis=0),
            jnp.concatenate([acc_q[k : k + 1, :] + acc_q[k + 1 : k + 2, :] for k in (4, 6)], axis=0),
        ],
        axis=1,
    )
    for parity in range(2):
        lanes = slice(parity * LANES, (parity + 1) * LANES)
        for y in range(4):
            part = [
                acc[k * HALF + y * OWN : k * HALF + (y + 1) * OWN, lanes] for k in range(5)
            ]
            piece = counts.at[parity, y]
            piece[:OWN, :] = part[0]
            piece[OWN : 2 * OWN, :] = part[1] + part[2]
            piece[2 * OWN : 3 * OWN, :] = part[3] + part[4]
            piece[3 * OWN :, :] = squares


def looked_up(tables, ids_col):
    slots = ids_col.shape[0]
    lane = lax.broadcasted_iota(I32, (slots, LANES), 1)
    in_row = (lax.broadcasted_iota(I32, (slots, 32), 1) == (ids_col >> 7)).astype(F32)
    cols = []
    for table in tables:
        picked = jnp.dot(
            in_row, table[...], precision=lax.Precision.HIGHEST, preferred_element_type=F32
        )
        cols.append(
            jnp.sum(jnp.where(lane == (ids_col & 127), picked, 0.0), axis=1, keepdims=True)
        )
    return cols


def kernel(
    ens, val, var, pnt, own, mean_tab, var_tab,
    out, post,
    ens_v, val_v, var_v, pnt_v, own_v, mean_v, ivar_v,
    rows_v, acc, acc_q, sums, counts, sums_core, counts_core, sums_to, counts_to, sums_chip, counts_chip, means, my_lam, lams, scale, to_region, from_region,
    load_sem, line_sem, all_sem, core_send, core_recv, chip_send, chip_recv,
    mean_send, mean_recv, lam_send, lam_recv, reg_send, reg_recv,
):
    loads = [
        pltpu.make_async_copy(a, b, load_sem.at[i])
        for i, (a, b) in enumerate(
            (
                (pnt, pnt_v),
                (val, val_v),
                (var, var_v),
                (ens, ens_v),
                (own, own_v),
                (mean_tab, mean_v),
                (var_tab, ivar_v),
            )
        )
    ]
    for load in loads:
        load.start()
    from_region[255:256, :] = jnp.zeros((1, LANES), F32)

    region, member = lax.axis_index("region"), lax.axis_index("member")
    y, core = lax.div(member, 2), lax.rem(member, 2)
    ys = [y, *(lax.rem(y + d, 4) for d in range(1, 4))]
    others = [2 * ys[d] + c for d in (2, 1, 3) for c in (core, 1 - core)] + [2 * y + 1 - core]
    x, z = lax.div(region, 8), lax.rem(region, 8)
    xs = [8 * lax.rem(x + d, 4) for d in range(4)]
    zs = [lax.rem(z + d, 8) for d in range(8)]
    along_x = [xs[d] + zs[0] for d in (2, 1, 3)]
    along_z = [xs[0] + zs[d] for d in (4, 3, 5, 2, 6, 1, 7)]
    members = [2 * ys[d] + c for d in range(4) for c in (core, 1 - core)]
    apart = sorted(
        (
            (-sum(min(a, n - a) for a, n in zip(d[:3], (4, 8, 4))), d)
            for d in ((dx, dz, dy, c) for dx in range(4) for dz in range(8) for dy in range(4) for c in range(2))
            if any(d)
        )
    )
    peers = [(xs[dx] + zs[dz], members[2 * dy + c]) for _, (dx, dz, dy, c) in apart]

    barrier = pltpu.get_barrier_semaphore()
    for peer in (along_x[0], *along_z[3:5]):
        pl.semaphore_signal(barrier, inc=1, device_id={"region": peer}, device_id_type=MESH)
    for peer in others:
        pl.semaphore_signal(barrier, inc=1, device_id={"member": peer}, device_id_type=MESH)
    for peer in (*along_x[1:], *along_z[5:]):
        pl.semaphore_signal(barrier, inc=1, device_id={"region": peer}, device_id_type=MESH)

    for load in loads[:3]:
        load.wait()
    histograms(val_v, var_v, pnt_v, rows_v, acc, acc_q, counts)

    for load in loads[3:]:
        load.wait()
    point_sums(ens_v, sums, 0, EARLY)
    pl.semaphore_wait(barrier, len(others) + len(along_x) + 4)

    def core_copy(k, d):
        return pltpu.make_async_remote_copy(
            src_ref=(sums, counts)[k].at[1 - core, ys[d]],
            dst_ref=(sums_core, counts_core)[k].at[d],
            send_sem=core_send.at[4 * k + d],
            recv_sem=core_recv.at[4 * k + d],
            device_id={"member": 2 * y + 1 - core},
            device_id_type=MESH,
        )

    def chip_copy(k, d, turn=0):
        i = 3 if turn else d - 1
        to = 1 - core if turn else core
        direct = k == 1 and d == 2
        return pltpu.make_async_remote_copy(
            src_ref=counts.at[to, ys[2]] if direct else (sums_to, counts_to)[k].at[d],
            dst_ref=(sums_chip, counts_chip)[k].at[i],
            send_sem=chip_send.at[4 * k + i],
            recv_sem=chip_recv.at[4 * k + i],
            device_id={"member": 2 * ys[d] + to},
            device_id_type=MESH,
        )

    chip_copies = [(1, 1, 0), (1, 3, 0), (0, 1, 0), (0, 3, 0), (1, 2, 0), (1, 2, 1), (0, 2, 0)]
    core_copies = [(1, 1), (1, 3), (0, 2), (0, 1), (0, 3), (1, 0), (0, 0)]

    for turn in range(2):
        chip_copy(1, 2, turn).start()
    for copy in core_copies:
        if copy[0]:
            core_copy(*copy).start()
    for peer in (*along_x, *along_z[3:5]):
        pl.semaphore_signal(line_sem, inc=1, device_id={"region": peer}, device_id_type=MESH)
    point_sums(ens_v, sums, EARLY, 16)
    for copy in core_copies:
        if not copy[0]:
            core_copy(*copy).start()
    for k, d in core_copies:
        own, came, total = ((sums, sums_core, sums_to), (counts, counts_core, counts_to))[k]
        core_copy(k, d).wait_recv()
        total[d] = own[core, ys[d]] + came[d]
        if d:
            chip_copy(k, d).start()
    pl.semaphore_wait(line_sem, len(along_x) + 2)
    for peer in along_z:
        pl.semaphore_signal(all_sem, inc=1, device_id={"region": peer}, device_id_type=MESH)

    sub = lax.broadcasted_iota(I32, (OWN, LANES), 0)
    lane = lax.broadcasted_iota(I32, (OWN, LANES), 1)
    ids_col = jnp.sum(
        jnp.where(lane == 2 * (OWN * y + sub) + core, own_v[...].astype(F32), 0.0),
        axis=1,
        keepdims=True,
    ).astype(I32)
    prior_mean, prior_var = looked_up((mean_v, ivar_v), ids_col)
    in_block = lane == (ids_col & 127)

    for copy in chip_copies:
        chip_copy(*copy).wait_recv()

    def summed(total, came, k, size=OWN):
        at = slice(k * OWN, k * OWN + size)
        terms = [came[i, at, :] for i in range(came.shape[0])]
        return total[0, at, :] + sum(terms[1:], terms[0])

    mean = summed(sums_to, sums_chip, 0) / 80.0
    first = core * HALF + y * OWN
    my_rows = pl.ds(pl.multiple_of(first, OWN), OWN)
    means[my_rows, :] = mean
    spread = (summed(sums_to, sums_chip, 1) - 80.0 * mean * mean) / 79.0
    count, value, error = (summed(counts_to, counts_chip, k) for k in range(3))
    squares = summed(counts_to, counts_chip, 3, 2)
    mine = lane == sub + first

    def per_slot(x):
        return jnp.sum(x, axis=1, keepdims=True)

    innov_sum = per_slot(
        jnp.where(mine, squares[0:1], 0.0)
        + mean * (count * mean - 2.0 * value)
    )
    error_error = per_slot(jnp.where(mine, squares[1:2], 0.0))
    count_spread = count * spread
    spread_sum = per_slot(count_spread)
    spread_spread = per_slot(count_spread * spread)
    spread_error = per_slot(spread * error)
    error_sum = per_slot(error)
    weight_var = (
        2.0 * prior_mean * prior_mean * (1.0 + spread_spread)
        + 4.0 * prior_mean * spread_error
        + 2.0 * error_error
    )
    lam = jnp.maximum(
        (prior_mean * weight_var + prior_var * spread_sum * (innov_sum - error_sum))
        / (weight_var + prior_var * spread_sum * spread_sum),
        1.0,
    )
    placed = jnp.where(in_block, lam, 0.0)
    for r in range(32):
        to_region[r] = jnp.sum(
            jnp.where((ids_col >> 7) == r, placed, 0.0), axis=0, keepdims=True
        )
    my_lam[...] = jnp.sum(jnp.where(mine, lam, 0.0), axis=0, keepdims=True)

    def to_all(some):
        for i, (peer, dest) in some:
            pltpu.make_async_remote_copy(
                src_ref=to_region.at[peer],
                dst_ref=from_region.at[pl.ds(i, 1)],
                send_sem=reg_send,
                recv_sem=reg_recv,
                device_id={"region": peer, "member": dest},
                device_id_type=MESH,
            ).start()

    everyone = list(enumerate(peers))
    pl.semaphore_wait(all_sem, len(along_z))
    to_all(everyone[:96])
    lam_copies = []
    for i, peer in enumerate(others):
        lam_copies.append(
            pltpu.make_async_remote_copy(
                src_ref=my_lam,
                dst_ref=lams.at[i],
                send_sem=lam_send.at[i],
                recv_sem=lam_recv.at[i],
                device_id={"member": peer},
                device_id_type=MESH,
            )
        )
        lam_copies[-1].start()
    mean_copies = []
    for i, peer in enumerate(others):
        mean_copies.append(
            pltpu.make_async_remote_copy(
                src_ref=means.at[my_rows],
                dst_ref=means.at[my_rows],
                send_sem=mean_send.at[i],
                recv_sem=mean_recv.at[i],
                device_id={"member": peer},
                device_id_type=MESH,
            )
        )
        mean_copies[-1].start()

    to_all(everyone[96:])
    for copy in lam_copies:
        copy.wait_recv()
    lam_row = my_lam[...]
    for i in range(len(others)):
        lam_row = lam_row + lams[i]
    eye = lax.broadcasted_iota(I32, (LANES, LANES), 0) == lax.broadcasted_iota(
        I32, (LANES, LANES), 1
    )
    lam_col = jnp.sum(jnp.where(eye, lam_row, 0.0), axis=1, keepdims=True)
    scale[...] = jnp.broadcast_to(jnp.sqrt(lam_col), (LANES, LANES))
    for copy in mean_copies:
        copy.wait_recv()

    @pl.loop(0, 16)
    def _(j):
        for i in range(8):
            at = pl.ds(pl.multiple_of(j * 1024 + i * LANES, LANES), LANES)
            row = pl.ds(HALF * (i % 2) + 4 * j + i // 2, 1)
            m = means[row, :]
            x = ens_v[:, at].astype(F32)
            out[:, at] = (m + scale[row, :] * (x - m)).astype(BF16)

    arrived = pltpu.make_async_remote_copy(
        src_ref=from_region.at[0:255],
        dst_ref=from_region.at[0:255],
        send_sem=reg_send,
        recv_sem=reg_recv,
        device_id={"member": others[0]},
        device_id_type=MESH,
    )
    for copy in core_copies:
        core_copy(*copy).wait_send()
    for copy in chip_copies:
        chip_copy(*copy).wait_send()
    for copy in (*mean_copies, *lam_copies, arrived):
        copy.wait_send()
    arrived.wait_recv()
    post_row = to_region[region] + jnp.sum(from_region[...], axis=0, keepdims=True)
    turned = pltpu.roll(jnp.broadcast_to(post_row, (8, LANES)), (8 - member) * OWN % LANES, 1)
    post[...] = turned[0:1, :OWN]


def written(a, b, a_out, b_out, sem):
    copies = [
        pltpu.make_async_copy(a, a_out, sem.at[0]),
        pltpu.make_async_copy(b, b_out, sem.at[1]),
    ]
    for copy in copies:
        copy.start()
    for copy in copies:
        copy.wait()


def body(ensemble, obs_value, obs_var, obs_point, owned_blocks, infl_mean, infl_var):
    anywhere = pl.BlockSpec(memory_space=pl.ANY)
    vmem = pl.BlockSpec(memory_space=pltpu.VMEM)
    dma = pltpu.SemaphoreType.DMA
    inflated, post = pl.pallas_call(
        kernel,
        out_shape=(pltpu.VMEM(ensemble.shape, BF16), pltpu.VMEM((1, OWN), F32)),
        in_specs=[anywhere] * 7,
        out_specs=(vmem, vmem),
        scratch_shapes=[
            pltpu.VMEM((10, 16384), BF16),
            pltpu.VMEM((32, LANES), F32),
            pltpu.VMEM((32, LANES), F32),
            pltpu.VMEM((32, LANES), I32),
            pltpu.VMEM((1, LANES), I32),
            pltpu.VMEM((32, LANES), F32),
            pltpu.VMEM((32, LANES), F32),
            pltpu.VMEM((14, 32, LANES), F32),
            pltpu.VMEM((5 * HALF, 2 * LANES), F32),
            pltpu.VMEM((8, HALF), F32),
            *[
                pltpu.VMEM((*lead, rows, LANES), F32)
                for lead in ((2, 4), (4,), (4,))
                for rows in (POINTS, COUNTS)
            ],
            pltpu.VMEM((3, POINTS, LANES), F32),
            pltpu.VMEM((4, COUNTS, LANES), F32),
            pltpu.VMEM((LANES, LANES), F32),
            pltpu.VMEM((1, LANES), F32),
            pltpu.VMEM((7, 1, LANES), F32),
            pltpu.VMEM((LANES, LANES), F32),
            pltpu.VMEM((32, 1, LANES), F32),
            pltpu.VMEM((256, LANES), F32),
            dma((7,)),
            pltpu.SemaphoreType.REGULAR,
            pltpu.SemaphoreType.REGULAR,
            *[dma((n,)) for n in (8, 8, 7, 7) for _ in range(2)],
            dma,
            dma,
        ],
        compiler_params=pltpu.CompilerParams(collective_id=0, has_side_effects=True),
    )(
        ensemble,
        obs_value,
        obs_var,
        obs_point,
        owned_blocks.reshape(1, -1),
        infl_mean.reshape(32, LANES),
        infl_var.reshape(32, LANES),
    )
    inflated, post = pl.pallas_call(
        written,
        out_shape=(
            jax.ShapeDtypeStruct(ensemble.shape, BF16),
            jax.ShapeDtypeStruct((1, OWN), F32),
        ),
        in_specs=(vmem, vmem),
        out_specs=(anywhere, anywhere),
        scratch_shapes=[dma((2,))],
    )(
        pltpu.with_memory_space_constraint(inflated, pltpu.VMEM),
        pltpu.with_memory_space_constraint(post, pltpu.VMEM),
    )
    return inflated, post.reshape(-1)


def solution(mesh):
    placed = (
        P("member", "region"),
        P(("region", "member"), None),
        P(("region", "member"), None),
        P(("region", "member"), None),
        P("region"),
        P(),
        P(),
    )
    return jax.shard_map(
        body,
        mesh=mesh,
        in_specs=placed,
        out_specs=(P("member", "region"), P(("region", "member"))),
        check_vma=False,
    )
```

```python
import jax
import jax.numpy as jnp
from jax import lax
from jax.experimental import pallas as pl
from jax.experimental.pallas import tpu as pltpu
from jax.sharding import PartitionSpec as P

MESH = pl.DeviceIdType.MESH
F32 = jnp.float32
BF16 = jnp.bfloat16
I32 = jnp.int32
OWN = 16
LANES = 128
HALF = 64
POINTS = 2 * OWN
COUNTS = 3 * OWN + 2
EARLY = 4
STEP = 32


def parts_of(x, count):
    parts = []
    for _ in range(count):
        parts.append(x.astype(BF16))
        x = x - parts[-1].astype(F32)
    return [p.astype(F32) for p in parts]


def point_sums(ens_v, sums, first, last):
    @pl.loop(first, last)
    def _(j):
        x = ens_v[:, pl.ds(pl.multiple_of(j * 1024, 1024), 1024)].astype(F32)
        total = jnp.sum(x, axis=0, keepdims=True)
        square = jnp.sum(x * x, axis=0, keepdims=True)
        for i in range(8):
            row = 4 * (j % 4) + i // 2
            piece = sums.at[i % 2, j // 4]
            piece[pl.ds(row, 1), :] = total[:, i * LANES : (i + 1) * LANES]
            piece[pl.ds(OWN + row, 1), :] = square[:, i * LANES : (i + 1) * LANES]


def tall(row, rows):
    same = jnp.broadcast_to(row, (16, LANES)).astype(BF16)
    return jnp.concatenate([same] * (rows // 16), axis=0)


def histograms(val_v, var_v, pnt_v, rows_v, acc, acc_q, counts):
    across = (((1,), (1,)), ((), ()))
    point, value, var = pnt_v[...], val_v[...], var_v[...]
    odd = ((point >> 7) & 1).astype(F32)
    squares = [*parts_of(value * value, 2), *parts_of(var * var, 2)]
    kinds = [
        (point >> 8).astype(F32),
        (point & 255).astype(F32),
        *parts_of(value, 2),
        *parts_of(var, 2),
        *(p * (1.0 - odd) for p in squares),
        *(p * odd for p in squares),
    ]
    for k, kind in enumerate(kinds):
        rows_v[k] = kind
    index = lax.broadcasted_iota(I32, (256, LANES), 0).astype(F32).astype(BF16)
    none, one = jnp.zeros((256, LANES), BF16), jnp.ones((256, LANES), BF16)
    sub = lax.broadcasted_iota(I32, (8, LANES), 0)

    def step(first):
        left, right, square = [], [], []
        for i in range(STEP):
            row = [rows_v[k, pl.ds(first + i, 1), :] for k in range(14)]
            in_high = index[:HALF] == tall(row[0], HALF)
            in_low = index == tall(row[1], 256)
            left.append(
                jnp.concatenate(
                    [
                        jnp.where(in_high, one[:HALF], none[:HALF]),
                        *(jnp.where(in_high, tall(w, HALF), none[:HALF]) for w in row[2:6]),
                    ],
                    axis=0,
                )
            )
            right.append(jnp.where(in_low, one, none))
            stack = jnp.broadcast_to(row[6], (8, LANES))
            for k in range(1, 8):
                stack = jnp.where(sub == k, row[6 + k], stack)
            square.append(stack)
        left = jnp.concatenate(left, axis=1)
        right = jnp.concatenate(right, axis=1)
        square = jnp.concatenate(square, axis=1).astype(BF16)
        return (
            lax.dot_general(left, right, across, preferred_element_type=F32),
            lax.dot_general(square, left[:HALF], across, preferred_element_type=F32),
        )

    if STEP == 32:
        acc[...], acc_q[...] = step(0)
    else:
        acc[...], acc_q[...] = jnp.zeros_like(acc), jnp.zeros_like(acc_q)

        @pl.loop(0, 32 // STEP)
        def _(i):
            more, more_q = step(i * STEP)
            acc[...] += more
            acc_q[...] += more_q

    squares = jnp.concatenate(
        [
            jnp.concatenate([acc_q[k : k + 1, :] + acc_q[k + 1 : k + 2, :] for k in (0, 2)], axis=0),
            jnp.concatenate([acc_q[k : k + 1, :] + acc_q[k + 1 : k + 2, :] for k in (4, 6)], axis=0),
        ],
        axis=1,
    )
    for parity in range(2):
        lanes = slice(parity * LANES, (parity + 1) * LANES)
        for y in range(4):
            part = [
                acc[k * HALF + y * OWN : k * HALF + (y + 1) * OWN, lanes] for k in range(5)
            ]
            piece = counts.at[parity, y]
            piece[:OWN, :] = part[0]
            piece[OWN : 2 * OWN, :] = part[1] + part[2]
            piece[2 * OWN : 3 * OWN, :] = part[3] + part[4]
            piece[3 * OWN :, :] = squares


def looked_up(tables, ids_col):
    slots = ids_col.shape[0]
    lane = lax.broadcasted_iota(I32, (slots, LANES), 1)
    in_row = (lax.broadcasted_iota(I32, (slots, 32), 1) == (ids_col >> 7)).astype(F32)
    cols = []
    for table in tables:
        picked = jnp.dot(
            in_row, table[...], precision=lax.Precision.HIGHEST, preferred_element_type=F32
        )
        cols.append(
            jnp.sum(jnp.where(lane == (ids_col & 127), picked, 0.0), axis=1, keepdims=True)
        )
    return cols


def kernel(
    ens, val, var, pnt, own, mean_tab, var_tab,
    out, post,
    ens_v, val_v, var_v, pnt_v, own_v, mean_v, ivar_v,
    rows_v, acc, acc_q, sums, counts, sums_core, counts_core, sums_to, counts_to, sums_chip, counts_chip, means, my_lam, lams, scale, to_region, from_region,
    load_sem, line_sem, all_sem, core_send, core_recv, chip_send, chip_recv,
    mean_send, mean_recv, lam_send, lam_recv, reg_send, reg_recv,
):
    loads = [
        pltpu.make_async_copy(a, b, load_sem.at[i])
        for i, (a, b) in enumerate(
            (
                (pnt, pnt_v),
                (val, val_v),
                (var, var_v),
                (ens, ens_v),
                (own, own_v),
                (mean_tab, mean_v),
                (var_tab, ivar_v),
            )
        )
    ]
    for load in loads:
        load.start()
    from_region[255:256, :] = jnp.zeros((1, LANES), F32)

    region, member = lax.axis_index("region"), lax.axis_index("member")
    y, core = lax.div(member, 2), lax.rem(member, 2)
    ys = [y, *(lax.rem(y + d, 4) for d in range(1, 4))]
    others = [2 * ys[d] + c for d in (2, 1, 3) for c in (core, 1 - core)] + [2 * y + 1 - core]
    x, z = lax.div(region, 8), lax.rem(region, 8)
    xs = [8 * lax.rem(x + d, 4) for d in range(4)]
    zs = [lax.rem(z + d, 8) for d in range(8)]
    along_x = [xs[d] + zs[0] for d in (2, 1, 3)]
    along_z = [xs[0] + zs[d] for d in (4, 3, 5, 2, 6, 1, 7)]
    members = [2 * ys[d] + c for d in range(4) for c in (core, 1 - core)]
    apart = sorted(
        (
            (-sum(min(a, n - a) for a, n in zip(d[:3], (4, 8, 4))), d)
            for d in ((dx, dz, dy, c) for dx in range(4) for dz in range(8) for dy in range(4) for c in range(2))
            if any(d)
        )
    )
    peers = [(xs[dx] + zs[dz], members[2 * dy + c]) for _, (dx, dz, dy, c) in apart]

    barrier = pltpu.get_barrier_semaphore()
    for peer in (along_x[0], *along_z[3:5]):
        pl.semaphore_signal(barrier, inc=1, device_id={"region": peer}, device_id_type=MESH)
    for peer in others:
        pl.semaphore_signal(barrier, inc=1, device_id={"member": peer}, device_id_type=MESH)
    for peer in (*along_x[1:], *along_z[5:]):
        pl.semaphore_signal(barrier, inc=1, device_id={"region": peer}, device_id_type=MESH)

    for load in loads[:3]:
        load.wait()
    histograms(val_v, var_v, pnt_v, rows_v, acc, acc_q, counts)

    for load in loads[3:]:
        load.wait()
    point_sums(ens_v, sums, 0, EARLY)
    pl.semaphore_wait(barrier, len(others) + len(along_x) + 4)

    def core_copy(k, d):
        return pltpu.make_async_remote_copy(
            src_ref=(sums, counts)[k].at[1 - core, ys[d]],
            dst_ref=(sums_core, counts_core)[k].at[d],
            send_sem=core_send.at[4 * k + d],
            recv_sem=core_recv.at[4 * k + d],
            device_id={"member": 2 * y + 1 - core},
            device_id_type=MESH,
        )

    def chip_copy(k, d, turn=0):
        i = 3 if turn else d - 1
        to = 1 - core if turn else core
        direct = k == 1 and d == 2
        return pltpu.make_async_remote_copy(
            src_ref=counts.at[to, ys[2]] if direct else (sums_to, counts_to)[k].at[d],
            dst_ref=(sums_chip, counts_chip)[k].at[i],
            send_sem=chip_send.at[4 * k + i],
            recv_sem=chip_recv.at[4 * k + i],
            device_id={"member": 2 * ys[d] + to},
            device_id_type=MESH,
        )

    chip_copies = [(1, 1, 0), (1, 3, 0), (0, 1, 0), (0, 3, 0), (1, 2, 0), (1, 2, 1), (0, 2, 0)]
    core_copies = [(1, 1), (1, 3), (0, 2), (0, 1), (0, 3), (1, 0), (0, 0)]

    for turn in range(2):
        chip_copy(1, 2, turn).start()
    for copy in core_copies:
        if copy[0]:
            core_copy(*copy).start()
    for peer in (*along_x, *along_z[3:5]):
        pl.semaphore_signal(line_sem, inc=1, device_id={"region": peer}, device_id_type=MESH)
    point_sums(ens_v, sums, EARLY, 16)
    for copy in core_copies:
        if not copy[0]:
            core_copy(*copy).start()
    for k, d in core_copies:
        own, came, total = ((sums, sums_core, sums_to), (counts, counts_core, counts_to))[k]
        core_copy(k, d).wait_recv()
        total[d] = own[core, ys[d]] + came[d]
        if d:
            chip_copy(k, d).start()
    pl.semaphore_wait(line_sem, len(along_x) + 2)
    for peer in along_z:
        pl.semaphore_signal(all_sem, inc=1, device_id={"region": peer}, device_id_type=MESH)

    sub = lax.broadcasted_iota(I32, (OWN, LANES), 0)
    lane = lax.broadcasted_iota(I32, (OWN, LANES), 1)
    ids_col = jnp.sum(
        jnp.where(lane == 2 * (OWN * y + sub) + core, own_v[...].astype(F32), 0.0),
        axis=1,
        keepdims=True,
    ).astype(I32)
    prior_mean, prior_var = looked_up((mean_v, ivar_v), ids_col)
    in_block = lane == (ids_col & 127)

    for copy in chip_copies:
        chip_copy(*copy).wait_recv()

    def summed(total, came, k, size=OWN):
        at = slice(k * OWN, k * OWN + size)
        terms = [came[i, at, :] for i in range(came.shape[0])]
        return total[0, at, :] + sum(terms[1:], terms[0])

    mean = summed(sums_to, sums_chip, 0) / 80.0
    first = core * HALF + y * OWN
    my_rows = pl.ds(pl.multiple_of(first, OWN), OWN)
    means[my_rows, :] = mean
    spread = (summed(sums_to, sums_chip, 1) - 80.0 * mean * mean) / 79.0
    count, value, error = (summed(counts_to, counts_chip, k) for k in range(3))
    squares = summed(counts_to, counts_chip, 3, 2)
    mine = lane == sub + first

    def per_slot(x):
        return jnp.sum(x, axis=1, keepdims=True)

    innov_sum = per_slot(
        jnp.where(mine, squares[0:1], 0.0)
        + mean * (count * mean - 2.0 * value)
    )
    error_error = per_slot(jnp.where(mine, squares[1:2], 0.0))
    count_spread = count * spread
    spread_sum = per_slot(count_spread)
    spread_spread = per_slot(count_spread * spread)
    spread_error = per_slot(spread * error)
    error_sum = per_slot(error)
    weight_var = (
        2.0 * prior_mean * prior_mean * (1.0 + spread_spread)
        + 4.0 * prior_mean * spread_error
        + 2.0 * error_error
    )
    lam = jnp.maximum(
        (prior_mean * weight_var + prior_var * spread_sum * (innov_sum - error_sum))
        / (weight_var + prior_var * spread_sum * spread_sum),
        1.0,
    )
    placed = jnp.where(in_block, lam, 0.0)
    for r in range(32):
        to_region[r] = jnp.sum(
            jnp.where((ids_col >> 7) == r, placed, 0.0), axis=0, keepdims=True
        )
    my_lam[...] = jnp.sum(jnp.where(mine, lam, 0.0), axis=0, keepdims=True)

    def to_all(some):
        for i, (peer, dest) in some:
            pltpu.make_async_remote_copy(
                src_ref=to_region.at[peer],
                dst_ref=from_region.at[pl.ds(i, 1)],
                send_sem=reg_send,
                recv_sem=reg_recv,
                device_id={"region": peer, "member": dest},
                device_id_type=MESH,
            ).start()

    everyone = list(enumerate(peers))
    pl.semaphore_wait(all_sem, len(along_z))
    to_all(everyone[:96])
    lam_copies = []
    for i, peer in enumerate(others):
        lam_copies.append(
            pltpu.make_async_remote_copy(
                src_ref=my_lam,
                dst_ref=lams.at[i],
                send_sem=lam_send.at[i],
                recv_sem=lam_recv.at[i],
                device_id={"member": peer},
                device_id_type=MESH,
            )
        )
        lam_copies[-1].start()
    to_all(everyone[96:])
    mean_copies = []
    for i, peer in enumerate(others):
        mean_copies.append(
            pltpu.make_async_remote_copy(
                src_ref=means.at[my_rows],
                dst_ref=means.at[my_rows],
                send_sem=mean_send.at[i],
                recv_sem=mean_recv.at[i],
                device_id={"member": peer},
                device_id_type=MESH,
            )
        )
        mean_copies[-1].start()

    for copy in lam_copies:
        copy.wait_recv()
    lam_row = my_lam[...]
    for i in range(len(others)):
        lam_row = lam_row + lams[i]
    eye = lax.broadcasted_iota(I32, (LANES, LANES), 0) == lax.broadcasted_iota(
        I32, (LANES, LANES), 1
    )
    lam_col = jnp.sum(jnp.where(eye, lam_row, 0.0), axis=1, keepdims=True)
    scale[...] = jnp.broadcast_to(jnp.sqrt(lam_col), (LANES, LANES))
    for copy in mean_copies:
        copy.wait_recv()

    @pl.loop(0, 16)
    def _(j):
        for i in range(8):
            at = pl.ds(pl.multiple_of(j * 1024 + i * LANES, LANES), LANES)
            row = pl.ds(HALF * (i % 2) + 4 * j + i // 2, 1)
            m = means[row, :]
            x = ens_v[:, at].astype(F32)
            out[:, at] = (m + scale[row, :] * (x - m)).astype(BF16)

    arrived = pltpu.make_async_remote_copy(
        src_ref=from_region.at[0:255],
        dst_ref=from_region.at[0:255],
        send_sem=reg_send,
        recv_sem=reg_recv,
        device_id={"member": others[0]},
        device_id_type=MESH,
    )
    for copy in core_copies:
        core_copy(*copy).wait_send()
    for copy in chip_copies:
        chip_copy(*copy).wait_send()
    for copy in (*mean_copies, *lam_copies, arrived):
        copy.wait_send()
    arrived.wait_recv()
    post_row = to_region[region] + jnp.sum(from_region[...], axis=0, keepdims=True)
    turned = pltpu.roll(jnp.broadcast_to(post_row, (8, LANES)), (8 - member) * OWN % LANES, 1)
    post[...] = turned[0:1, :OWN]


def written(a, b, a_out, b_out, sem):
    copies = [
        pltpu.make_async_copy(a, a_out, sem.at[0]),
        pltpu.make_async_copy(b, b_out, sem.at[1]),
    ]
    for copy in copies:
        copy.start()
    for copy in copies:
        copy.wait()


def body(ensemble, obs_value, obs_var, obs_point, owned_blocks, infl_mean, infl_var):
    anywhere = pl.BlockSpec(memory_space=pl.ANY)
    vmem = pl.BlockSpec(memory_space=pltpu.VMEM)
    dma = pltpu.SemaphoreType.DMA
    inflated, post = pl.pallas_call(
        kernel,
        out_shape=(pltpu.VMEM(ensemble.shape, BF16), pltpu.VMEM((1, OWN), F32)),
        in_specs=[anywhere] * 7,
        out_specs=(vmem, vmem),
        scratch_shapes=[
            pltpu.VMEM((10, 16384), BF16),
            pltpu.VMEM((32, LANES), F32),
            pltpu.VMEM((32, LANES), F32),
            pltpu.VMEM((32, LANES), I32),
            pltpu.VMEM((1, LANES), I32),
            pltpu.VMEM((32, LANES), F32),
            pltpu.VMEM((32, LANES), F32),
            pltpu.VMEM((14, 32, LANES), F32),
            pltpu.VMEM((5 * HALF, 2 * LANES), F32),
            pltpu.VMEM((8, HALF), F32),
            *[
                pltpu.VMEM((*lead, rows, LANES), F32)
                for lead in ((2, 4), (4,), (4,))
                for rows in (POINTS, COUNTS)
            ],
            pltpu.VMEM((3, POINTS, LANES), F32),
            pltpu.VMEM((4, COUNTS, LANES), F32),
            pltpu.VMEM((LANES, LANES), F32),
            pltpu.VMEM((1, LANES), F32),
            pltpu.VMEM((7, 1, LANES), F32),
            pltpu.VMEM((LANES, LANES), F32),
            pltpu.VMEM((32, 1, LANES), F32),
            pltpu.VMEM((256, LANES), F32),
            dma((7,)),
            pltpu.SemaphoreType.REGULAR,
            pltpu.SemaphoreType.REGULAR,
            *[dma((n,)) for n in (8, 8, 7, 7) for _ in range(2)],
            dma,
            dma,
        ],
        compiler_params=pltpu.CompilerParams(collective_id=0, has_side_effects=True),
    )(
        ensemble,
        obs_value,
        obs_var,
        obs_point,
        owned_blocks.reshape(1, -1),
        infl_mean.reshape(32, LANES),
        infl_var.reshape(32, LANES),
    )
    inflated, post = pl.pallas_call(
        written,
        out_shape=(
            jax.ShapeDtypeStruct(ensemble.shape, BF16),
            jax.ShapeDtypeStruct((1, OWN), F32),
        ),
        in_specs=(vmem, vmem),
        out_specs=(anywhere, anywhere),
        scratch_shapes=[dma((2,))],
    )(
        pltpu.with_memory_space_constraint(inflated, pltpu.VMEM),
        pltpu.with_memory_space_constraint(post, pltpu.VMEM),
    )
    return inflated, post.reshape(-1)


def solution(mesh):
    placed = (
        P("member", "region"),
        P(("region", "member"), None),
        P(("region", "member"), None),
        P(("region", "member"), None),
        P("region"),
        P(),
        P(),
    )
    return jax.shard_map(
        body,
        mesh=mesh,
        in_specs=placed,
        out_specs=(P("member", "region"), P(("region", "member"))),
        check_vma=False,
    )
```

```python
import jax
import jax.numpy as jnp
from jax import lax
from jax.experimental import pallas as pl
from jax.experimental.pallas import tpu as pltpu
from jax.sharding import PartitionSpec as P

MESH = pl.DeviceIdType.MESH
F32 = jnp.float32
BF16 = jnp.bfloat16
I32 = jnp.int32
OWN = 16
LANES = 128
HALF = 64
POINTS = 2 * OWN
COUNTS = 3 * OWN + 2
EARLY = 4
STEP = 32


def parts_of(x, count):
    parts = []
    for _ in range(count):
        parts.append(x.astype(BF16))
        x = x - parts[-1].astype(F32)
    return [p.astype(F32) for p in parts]


def point_sums(ens_v, sums, first, last):
    @pl.loop(first, last)
    def _(j):
        x = ens_v[:, pl.ds(pl.multiple_of(j * 1024, 1024), 1024)].astype(F32)
        total = jnp.sum(x, axis=0, keepdims=True)
        square = jnp.sum(x * x, axis=0, keepdims=True)
        for i in range(8):
            row = 4 * (j % 4) + i // 2
            piece = sums.at[i % 2, j // 4]
            piece[pl.ds(row, 1), :] = total[:, i * LANES : (i + 1) * LANES]
            piece[pl.ds(OWN + row, 1), :] = square[:, i * LANES : (i + 1) * LANES]


def tall(row, rows):
    same = jnp.broadcast_to(row, (16, LANES)).astype(BF16)
    return jnp.concatenate([same] * (rows // 16), axis=0)


def histograms(val_v, var_v, pnt_v, rows_v, acc, acc_q, counts):
    across = (((1,), (1,)), ((), ()))
    point, value, var = pnt_v[...], val_v[...], var_v[...]
    odd = ((point >> 7) & 1).astype(F32)
    squares = [*parts_of(value * value, 2), *parts_of(var * var, 2)]
    kinds = [
        (point >> 8).astype(F32),
        (point & 255).astype(F32),
        *parts_of(value, 2),
        *parts_of(var, 2),
        *(p * (1.0 - odd) for p in squares),
        *(p * odd for p in squares),
    ]
    for k, kind in enumerate(kinds):
        rows_v[k] = kind
    index = lax.broadcasted_iota(I32, (256, LANES), 0).astype(F32).astype(BF16)
    none, one = jnp.zeros((256, LANES), BF16), jnp.ones((256, LANES), BF16)
    sub = lax.broadcasted_iota(I32, (8, LANES), 0)

    def step(first):
        left, right, square = [], [], []
        for i in range(STEP):
            row = [rows_v[k, pl.ds(first + i, 1), :] for k in range(14)]
            in_high = index[:HALF] == tall(row[0], HALF)
            in_low = index == tall(row[1], 256)
            left.append(
                jnp.concatenate(
                    [
                        jnp.where(in_high, one[:HALF], none[:HALF]),
                        *(jnp.where(in_high, tall(w, HALF), none[:HALF]) for w in row[2:6]),
                    ],
                    axis=0,
                )
            )
            right.append(jnp.where(in_low, one, none))
            stack = jnp.broadcast_to(row[6], (8, LANES))
            for k in range(1, 8):
                stack = jnp.where(sub == k, row[6 + k], stack)
            square.append(stack)
        left = jnp.concatenate(left, axis=1)
        right = jnp.concatenate(right, axis=1)
        square = jnp.concatenate(square, axis=1).astype(BF16)
        return (
            lax.dot_general(left, right, across, preferred_element_type=F32),
            lax.dot_general(square, left[:HALF], across, preferred_element_type=F32),
        )

    if STEP == 32:
        acc[...], acc_q[...] = step(0)
    else:
        acc[...], acc_q[...] = jnp.zeros_like(acc), jnp.zeros_like(acc_q)

        @pl.loop(0, 32 // STEP)
        def _(i):
            more, more_q = step(i * STEP)
            acc[...] += more
            acc_q[...] += more_q

    squares = jnp.concatenate(
        [
            jnp.concatenate([acc_q[k : k + 1, :] + acc_q[k + 1 : k + 2, :] for k in (0, 2)], axis=0),
            jnp.concatenate([acc_q[k : k + 1, :] + acc_q[k + 1 : k + 2, :] for k in (4, 6)], axis=0),
        ],
        axis=1,
    )
    for parity in range(2):
        lanes = slice(parity * LANES, (parity + 1) * LANES)
        for y in range(4):
            part = [
                acc[k * HALF + y * OWN : k * HALF + (y + 1) * OWN, lanes] for k in range(5)
            ]
            piece = counts.at[parity, y]
            piece[:OWN, :] = part[0]
            piece[OWN : 2 * OWN, :] = part[1] + part[2]
            piece[2 * OWN : 3 * OWN, :] = part[3] + part[4]
            piece[3 * OWN :, :] = squares


def looked_up(tables, ids_col):
    slots = ids_col.shape[0]
    lane = lax.broadcasted_iota(I32, (slots, LANES), 1)
    in_row = (lax.broadcasted_iota(I32, (slots, 32), 1) == (ids_col >> 7)).astype(F32)
    cols = []
    for table in tables:
        picked = jnp.dot(
            in_row, table[...], precision=lax.Precision.HIGHEST, preferred_element_type=F32
        )
        cols.append(
            jnp.sum(jnp.where(lane == (ids_col & 127), picked, 0.0), axis=1, keepdims=True)
        )
    return cols


def kernel(
    ens, val, var, pnt, own, mean_tab, var_tab,
    out, post,
    ens_v, val_v, var_v, pnt_v, own_v, mean_v, ivar_v,
    rows_v, acc, acc_q, sums, counts, sums_core, counts_core, sums_to, counts_to, sums_chip, counts_chip, means, my_lam, lams, scale, to_region, from_region,
    load_sem, line_sem, all_sem, core_send, core_recv, chip_send, chip_recv,
    mean_send, mean_recv, lam_send, lam_recv, reg_send, reg_recv,
):
    loads = [
        pltpu.make_async_copy(a, b, load_sem.at[i])
        for i, (a, b) in enumerate(
            (
                (pnt, pnt_v),
                (val, val_v),
                (var, var_v),
                (ens, ens_v),
                (own, own_v),
                (mean_tab, mean_v),
                (var_tab, ivar_v),
            )
        )
    ]
    for load in loads:
        load.start()
    from_region[255:256, :] = jnp.zeros((1, LANES), F32)

    region, member = lax.axis_index("region"), lax.axis_index("member")
    barrier = pltpu.get_barrier_semaphore()

    def greet(**peer):
        pl.semaphore_signal(barrier, inc=1, device_id=peer, device_id_type=MESH)

    x, z = lax.div(region, 8), lax.rem(region, 8)
    zs = [z, *(lax.rem(z + d, 8) for d in range(1, 8))]
    along_z = [8 * x + zs[d] for d in (4, 3, 5, 2, 6, 1, 7)]
    for peer in along_z[3:5]:
        greet(region=peer)
    xs = [8 * x, *(8 * lax.rem(x + d, 4) for d in range(1, 4))]
    along_x = [xs[d] + z for d in (2, 1, 3)]
    greet(region=along_x[0])
    y, core = lax.div(member, 2), lax.rem(member, 2)
    ys = [y, *(lax.rem(y + d, 4) for d in range(1, 4))]
    others = [2 * ys[d] + c for d in (2, 1, 3) for c in (core, 1 - core)] + [2 * y + 1 - core]
    for peer in others:
        greet(member=peer)
    for peer in (*along_x[1:], *along_z[5:]):
        greet(region=peer)
    members = [2 * ys[d] + c for d in range(4) for c in (core, 1 - core)]
    apart = sorted(
        (
            (-sum(min(a, n - a) for a, n in zip(d[:3], (4, 8, 4))), d)
            for d in ((dx, dz, dy, c) for dx in range(4) for dz in range(8) for dy in range(4) for c in range(2))
            if any(d)
        )
    )
    peers = [(xs[dx] + zs[dz], members[2 * dy + c]) for _, (dx, dz, dy, c) in apart]

    for load in loads[:3]:
        load.wait()
    histograms(val_v, var_v, pnt_v, rows_v, acc, acc_q, counts)

    for load in loads[3:]:
        load.wait()
    point_sums(ens_v, sums, 0, EARLY)
    pl.semaphore_wait(barrier, len(others) + len(along_x) + 4)

    def core_copy(k, d):
        return pltpu.make_async_remote_copy(
            src_ref=(sums, counts)[k].at[1 - core, ys[d]],
            dst_ref=(sums_core, counts_core)[k].at[d],
            send_sem=core_send.at[4 * k + d],
            recv_sem=core_recv.at[4 * k + d],
            device_id={"member": 2 * y + 1 - core},
            device_id_type=MESH,
        )

    def chip_copy(k, d, turn=0):
        i = 3 if turn else d - 1
        to = 1 - core if turn else core
        direct = k == 1 and d == 2
        return pltpu.make_async_remote_copy(
            src_ref=counts.at[to, ys[2]] if direct else (sums_to, counts_to)[k].at[d],
            dst_ref=(sums_chip, counts_chip)[k].at[i],
            send_sem=chip_send.at[4 * k + i],
            recv_sem=chip_recv.at[4 * k + i],
            device_id={"member": 2 * ys[d] + to},
            device_id_type=MESH,
        )

    chip_copies = [(1, 1, 0), (1, 3, 0), (0, 1, 0), (0, 3, 0), (1, 2, 0), (1, 2, 1), (0, 2, 0)]
    core_copies = [(1, 1), (1, 3), (0, 2), (0, 1), (0, 3), (1, 0), (0, 0)]

    for turn in range(2):
        chip_copy(1, 2, turn).start()
    for copy in core_copies:
        if copy[0]:
            core_copy(*copy).start()
    for peer in (*along_x, *along_z[3:5]):
        pl.semaphore_signal(line_sem, inc=1, device_id={"region": peer}, device_id_type=MESH)
    point_sums(ens_v, sums, EARLY, 16)
    for copy in core_copies:
        if not copy[0]:
            core_copy(*copy).start()
    for k, d in core_copies:
        own, came, total = ((sums, sums_core, sums_to), (counts, counts_core, counts_to))[k]
        core_copy(k, d).wait_recv()
        total[d] = own[core, ys[d]] + came[d]
        if d:
            chip_copy(k, d).start()
    pl.semaphore_wait(line_sem, len(along_x) + 2)
    for peer in along_z:
        pl.semaphore_signal(all_sem, inc=1, device_id={"region": peer}, device_id_type=MESH)

    sub = lax.broadcasted_iota(I32, (OWN, LANES), 0)
    lane = lax.broadcasted_iota(I32, (OWN, LANES), 1)
    ids_col = jnp.sum(
        jnp.where(lane == 2 * (OWN * y + sub) + core, own_v[...].astype(F32), 0.0),
        axis=1,
        keepdims=True,
    ).astype(I32)
    prior_mean, prior_var = looked_up((mean_v, ivar_v), ids_col)
    in_block = lane == (ids_col & 127)

    for copy in chip_copies:
        chip_copy(*copy).wait_recv()

    def summed(total, came, k, size=OWN):
        at = slice(k * OWN, k * OWN + size)
        terms = [came[i, at, :] for i in range(came.shape[0])]
        return total[0, at, :] + sum(terms[1:], terms[0])

    mean = summed(sums_to, sums_chip, 0) / 80.0
    first = core * HALF + y * OWN
    my_rows = pl.ds(pl.multiple_of(first, OWN), OWN)
    means[my_rows, :] = mean
    spread = (summed(sums_to, sums_chip, 1) - 80.0 * mean * mean) / 79.0
    count, value, error = (summed(counts_to, counts_chip, k) for k in range(3))
    squares = summed(counts_to, counts_chip, 3, 2)
    mine = lane == sub + first

    def per_slot(x):
        return jnp.sum(x, axis=1, keepdims=True)

    innov_sum = per_slot(
        jnp.where(mine, squares[0:1], 0.0)
        + mean * (count * mean - 2.0 * value)
    )
    error_error = per_slot(jnp.where(mine, squares[1:2], 0.0))
    count_spread = count * spread
    spread_sum = per_slot(count_spread)
    spread_spread = per_slot(count_spread * spread)
    spread_error = per_slot(spread * error)
    error_sum = per_slot(error)
    weight_var = (
        2.0 * prior_mean * prior_mean * (1.0 + spread_spread)
        + 4.0 * prior_mean * spread_error
        + 2.0 * error_error
    )
    lam = jnp.maximum(
        (prior_mean * weight_var + prior_var * spread_sum * (innov_sum - error_sum))
        / (weight_var + prior_var * spread_sum * spread_sum),
        1.0,
    )
    placed = jnp.where(in_block, lam, 0.0)
    for r in range(32):
        to_region[r] = jnp.sum(
            jnp.where((ids_col >> 7) == r, placed, 0.0), axis=0, keepdims=True
        )
    my_lam[...] = jnp.sum(jnp.where(mine, lam, 0.0), axis=0, keepdims=True)

    def to_all(some):
        for i, (peer, dest) in some:
            pltpu.make_async_remote_copy(
                src_ref=to_region.at[peer],
                dst_ref=from_region.at[pl.ds(i, 1)],
                send_sem=reg_send,
                recv_sem=reg_recv,
                device_id={"region": peer, "member": dest},
                device_id_type=MESH,
            ).start()

    everyone = list(enumerate(peers))
    pl.semaphore_wait(all_sem, len(along_z))
    to_all(everyone[:96])
    lam_copies = []
    for i, peer in enumerate(others):
        lam_copies.append(
            pltpu.make_async_remote_copy(
                src_ref=my_lam,
                dst_ref=lams.at[i],
                send_sem=lam_send.at[i],
                recv_sem=lam_recv.at[i],
                device_id={"member": peer},
                device_id_type=MESH,
            )
        )
        lam_copies[-1].start()
    to_all(everyone[96:])
    mean_copies = []
    for i, peer in enumerate(others):
        mean_copies.append(
            pltpu.make_async_remote_copy(
                src_ref=means.at[my_rows],
                dst_ref=means.at[my_rows],
                send_sem=mean_send.at[i],
                recv_sem=mean_recv.at[i],
                device_id={"member": peer},
                device_id_type=MESH,
            )
        )
        mean_copies[-1].start()

    for copy in lam_copies:
        copy.wait_recv()
    lam_row = my_lam[...]
    for i in range(len(others)):
        lam_row = lam_row + lams[i]
    eye = lax.broadcasted_iota(I32, (LANES, LANES), 0) == lax.broadcasted_iota(
        I32, (LANES, LANES), 1
    )
    lam_col = jnp.sum(jnp.where(eye, lam_row, 0.0), axis=1, keepdims=True)
    scale[...] = jnp.broadcast_to(jnp.sqrt(lam_col), (LANES, LANES))
    for copy in mean_copies:
        copy.wait_recv()

    @pl.loop(0, 16)
    def _(j):
        for i in range(8):
            at = pl.ds(pl.multiple_of(j * 1024 + i * LANES, LANES), LANES)
            row = pl.ds(HALF * (i % 2) + 4 * j + i // 2, 1)
            m = means[row, :]
            x = ens_v[:, at].astype(F32)
            out[:, at] = (m + scale[row, :] * (x - m)).astype(BF16)

    arrived = pltpu.make_async_remote_copy(
        src_ref=from_region.at[0:255],
        dst_ref=from_region.at[0:255],
        send_sem=reg_send,
        recv_sem=reg_recv,
        device_id={"member": others[0]},
        device_id_type=MESH,
    )
    for copy in core_copies:
        core_copy(*copy).wait_send()
    for copy in chip_copies:
        chip_copy(*copy).wait_send()
    for copy in (*mean_copies, *lam_copies, arrived):
        copy.wait_send()
    arrived.wait_recv()
    post_row = to_region[region] + jnp.sum(from_region[...], axis=0, keepdims=True)
    turned = pltpu.roll(jnp.broadcast_to(post_row, (8, LANES)), (8 - member) * OWN % LANES, 1)
    post[...] = turned[0:1, :OWN]


def written(a, b, a_out, b_out, sem):
    copies = [
        pltpu.make_async_copy(a, a_out, sem.at[0]),
        pltpu.make_async_copy(b, b_out, sem.at[1]),
    ]
    for copy in copies:
        copy.start()
    for copy in copies:
        copy.wait()


def body(ensemble, obs_value, obs_var, obs_point, owned_blocks, infl_mean, infl_var):
    anywhere = pl.BlockSpec(memory_space=pl.ANY)
    vmem = pl.BlockSpec(memory_space=pltpu.VMEM)
    dma = pltpu.SemaphoreType.DMA
    inflated, post = pl.pallas_call(
        kernel,
        out_shape=(pltpu.VMEM(ensemble.shape, BF16), pltpu.VMEM((1, OWN), F32)),
        in_specs=[anywhere] * 7,
        out_specs=(vmem, vmem),
        scratch_shapes=[
            pltpu.VMEM((10, 16384), BF16),
            pltpu.VMEM((32, LANES), F32),
            pltpu.VMEM((32, LANES), F32),
            pltpu.VMEM((32, LANES), I32),
            pltpu.VMEM((1, LANES), I32),
            pltpu.VMEM((32, LANES), F32),
            pltpu.VMEM((32, LANES), F32),
            pltpu.VMEM((14, 32, LANES), F32),
            pltpu.VMEM((5 * HALF, 2 * LANES), F32),
            pltpu.VMEM((8, HALF), F32),
            *[
                pltpu.VMEM((*lead, rows, LANES), F32)
                for lead in ((2, 4), (4,), (4,))
                for rows in (POINTS, COUNTS)
            ],
            pltpu.VMEM((3, POINTS, LANES), F32),
            pltpu.VMEM((4, COUNTS, LANES), F32),
            pltpu.VMEM((LANES, LANES), F32),
            pltpu.VMEM((1, LANES), F32),
            pltpu.VMEM((7, 1, LANES), F32),
            pltpu.VMEM((LANES, LANES), F32),
            pltpu.VMEM((32, 1, LANES), F32),
            pltpu.VMEM((256, LANES), F32),
            dma((7,)),
            pltpu.SemaphoreType.REGULAR,
            pltpu.SemaphoreType.REGULAR,
            *[dma((n,)) for n in (8, 8, 7, 7) for _ in range(2)],
            dma,
            dma,
        ],
        compiler_params=pltpu.CompilerParams(collective_id=0, has_side_effects=True),
    )(
        ensemble,
        obs_value,
        obs_var,
        obs_point,
        owned_blocks.reshape(1, -1),
        infl_mean.reshape(32, LANES),
        infl_var.reshape(32, LANES),
    )
    inflated, post = pl.pallas_call(
        written,
        out_shape=(
            jax.ShapeDtypeStruct(ensemble.shape, BF16),
            jax.ShapeDtypeStruct((1, OWN), F32),
        ),
        in_specs=(vmem, vmem),
        out_specs=(anywhere, anywhere),
        scratch_shapes=[dma((2,))],
    )(
        pltpu.with_memory_space_constraint(inflated, pltpu.VMEM),
        pltpu.with_memory_space_constraint(post, pltpu.VMEM),
    )
    return inflated, post.reshape(-1)


def solution(mesh):
    placed = (
        P("member", "region"),
        P(("region", "member"), None),
        P(("region", "member"), None),
        P(("region", "member"), None),
        P("region"),
        P(),
        P(),
    )
    return jax.shard_map(
        body,
        mesh=mesh,
        in_specs=placed,
        out_specs=(P("member", "region"), P(("region", "member"))),
        check_vma=False,
    )
```

```python
import jax
import jax.numpy as jnp
from jax import lax
from jax.experimental import pallas as pl
from jax.experimental.pallas import tpu as pltpu
from jax.sharding import PartitionSpec as P

MESH = pl.DeviceIdType.MESH
F32 = jnp.float32
BF16 = jnp.bfloat16
I32 = jnp.int32
OWN = 16
LANES = 128
HALF = 64
POINTS = 2 * OWN
COUNTS = 3 * OWN + 2
EARLY = 4
STEP = 32


def parts_of(x, count):
    parts = []
    for _ in range(count):
        parts.append(x.astype(BF16))
        x = x - parts[-1].astype(F32)
    return [p.astype(F32) for p in parts]


def point_sums(ens_v, sums, first, last):
    @pl.loop(first, last)
    def _(j):
        x = ens_v[:, pl.ds(pl.multiple_of(j * 1024, 1024), 1024)].astype(F32)
        total = jnp.sum(x, axis=0, keepdims=True)
        square = jnp.sum(x * x, axis=0, keepdims=True)
        for i in range(8):
            row = 4 * (j % 4) + i // 2
            piece = sums.at[i % 2, j // 4]
            piece[pl.ds(row, 1), :] = total[:, i * LANES : (i + 1) * LANES]
            piece[pl.ds(OWN + row, 1), :] = square[:, i * LANES : (i + 1) * LANES]


def tall(row, rows):
    same = jnp.broadcast_to(row, (16, LANES)).astype(BF16)
    return jnp.concatenate([same] * (rows // 16), axis=0)


def histograms(val_v, var_v, pnt_v, rows_v, acc, acc_q, counts):
    across = (((1,), (1,)), ((), ()))
    point, value, var = pnt_v[...], val_v[...], var_v[...]
    odd = ((point >> 7) & 1).astype(F32)
    squares = [*parts_of(value * value, 2), *parts_of(var * var, 2)]
    kinds = [
        (point >> 8).astype(F32),
        (point & 255).astype(F32),
        *parts_of(value, 2),
        *parts_of(var, 2),
        *(p * (1.0 - odd) for p in squares),
        *(p * odd for p in squares),
    ]
    for k, kind in enumerate(kinds):
        rows_v[k] = kind
    index = lax.broadcasted_iota(I32, (256, LANES), 0).astype(F32).astype(BF16)
    none, one = jnp.zeros((256, LANES), BF16), jnp.ones((256, LANES), BF16)
    sub = lax.broadcasted_iota(I32, (8, LANES), 0)

    def step(first):
        left, right, square = [], [], []
        for i in range(STEP):
            row = [rows_v[k, pl.ds(first + i, 1), :] for k in range(14)]
            in_high = index[:HALF] == tall(row[0], HALF)
            in_low = index == tall(row[1], 256)
            left.append(
                jnp.concatenate(
                    [
                        jnp.where(in_high, one[:HALF], none[:HALF]),
                        *(jnp.where(in_high, tall(w, HALF), none[:HALF]) for w in row[2:6]),
                    ],
                    axis=0,
                )
            )
            right.append(jnp.where(in_low, one, none))
            stack = jnp.broadcast_to(row[6], (8, LANES))
            for k in range(1, 8):
                stack = jnp.where(sub == k, row[6 + k], stack)
            square.append(stack)
        left = jnp.concatenate(left, axis=1)
        right = jnp.concatenate(right, axis=1)
        square = jnp.concatenate(square, axis=1).astype(BF16)
        return (
            lax.dot_general(left, right, across, preferred_element_type=F32),
            lax.dot_general(square, left[:HALF], across, preferred_element_type=F32),
        )

    if STEP == 32:
        acc[...], acc_q[...] = step(0)
    else:
        acc[...], acc_q[...] = jnp.zeros_like(acc), jnp.zeros_like(acc_q)

        @pl.loop(0, 32 // STEP)
        def _(i):
            more, more_q = step(i * STEP)
            acc[...] += more
            acc_q[...] += more_q

    squares = jnp.concatenate(
        [
            jnp.concatenate([acc_q[k : k + 1, :] + acc_q[k + 1 : k + 2, :] for k in (0, 2)], axis=0),
            jnp.concatenate([acc_q[k : k + 1, :] + acc_q[k + 1 : k + 2, :] for k in (4, 6)], axis=0),
        ],
        axis=1,
    )
    for parity in range(2):
        lanes = slice(parity * LANES, (parity + 1) * LANES)
        for y in range(4):
            part = [
                acc[k * HALF + y * OWN : k * HALF + (y + 1) * OWN, lanes] for k in range(5)
            ]
            piece = counts.at[parity, y]
            piece[:OWN, :] = part[0]
            piece[OWN : 2 * OWN, :] = part[1] + part[2]
            piece[2 * OWN : 3 * OWN, :] = part[3] + part[4]
            piece[3 * OWN :, :] = squares


def looked_up(tables, ids_col):
    slots = ids_col.shape[0]
    lane = lax.broadcasted_iota(I32, (slots, LANES), 1)
    in_row = (lax.broadcasted_iota(I32, (slots, 32), 1) == (ids_col >> 7)).astype(F32)
    cols = []
    for table in tables:
        picked = jnp.dot(
            in_row, table[...], precision=lax.Precision.HIGHEST, preferred_element_type=F32
        )
        cols.append(
            jnp.sum(jnp.where(lane == (ids_col & 127), picked, 0.0), axis=1, keepdims=True)
        )
    return cols


def kernel(
    ens, val, var, pnt, own, mean_tab, var_tab,
    out, post,
    ens_v, val_v, var_v, pnt_v, own_v, mean_v, ivar_v,
    rows_v, acc, acc_q, sums, counts, sums_core, counts_core, sums_to, counts_to, sums_chip, counts_chip, means, my_lam, lams, scale, to_region, from_region,
    load_sem, line_sem, all_sem, core_send, core_recv, chip_send, chip_recv,
    mean_send, mean_recv, lam_send, lam_recv, reg_send, reg_recv,
):
    loads = [
        pltpu.make_async_copy(a, b, load_sem.at[i])
        for i, (a, b) in enumerate(
            (
                (pnt, pnt_v),
                (val, val_v),
                (var, var_v),
                (ens, ens_v),
                (own, own_v),
                (mean_tab, mean_v),
                (var_tab, ivar_v),
            )
        )
    ]
    for load in loads:
        load.start()
    from_region[255:256, :] = jnp.zeros((1, LANES), F32)

    region, member = lax.axis_index("region"), lax.axis_index("member")
    y, core = lax.div(member, 2), lax.rem(member, 2)
    ys = [y, *(lax.rem(y + d, 4) for d in range(1, 4))]
    others = [2 * ys[d] + c for d in (2, 1, 3) for c in (core, 1 - core)] + [2 * y + 1 - core]
    x, z = lax.div(region, 8), lax.rem(region, 8)
    xs = [8 * lax.rem(x + d, 4) for d in range(4)]
    zs = [lax.rem(z + d, 8) for d in range(8)]
    along_x = [xs[d] + zs[0] for d in (2, 1, 3)]
    along_z = [xs[0] + zs[d] for d in (4, 3, 5, 2, 6, 1, 7)]
    members = [2 * ys[d] + c for d in range(4) for c in (core, 1 - core)]
    apart = sorted(
        (
            (-sum(min(a, n - a) for a, n in zip(d[:3], (4, 8, 4))), d)
            for d in ((dx, dz, dy, c) for dx in range(4) for dz in range(8) for dy in range(4) for c in range(2))
            if any(d)
        )
    )
    peers = [(xs[dx] + zs[dz], members[2 * dy + c]) for _, (dx, dz, dy, c) in apart]

    barrier = pltpu.get_barrier_semaphore()
    for peer in (along_x[0], *along_z[3:5]):
        pl.semaphore_signal(barrier, inc=1, device_id={"region": peer}, device_id_type=MESH)
    for peer in others:
        pl.semaphore_signal(barrier, inc=1, device_id={"member": peer}, device_id_type=MESH)
    for peer in (*along_x[1:], *along_z[5:]):
        pl.semaphore_signal(barrier, inc=1, device_id={"region": peer}, device_id_type=MESH)

    for load in loads[:3]:
        load.wait()
    histograms(val_v, var_v, pnt_v, rows_v, acc, acc_q, counts)

    for load in loads[3:]:
        load.wait()
    point_sums(ens_v, sums, 0, EARLY)
    pl.semaphore_wait(barrier, len(others) + len(along_x) + 4)

    def core_copy(k, d):
        return pltpu.make_async_remote_copy(
            src_ref=(sums, counts)[k].at[1 - core, ys[d]],
            dst_ref=(sums_core, counts_core)[k].at[d],
            send_sem=core_send.at[4 * k + d],
            recv_sem=core_recv.at[4 * k + d],
            device_id={"member": 2 * y + 1 - core},
            device_id_type=MESH,
        )

    def chip_copy(k, d, turn=0):
        i = 3 if turn else d - 1
        to = 1 - core if turn else core
        direct = k == 1 and d == 2
        return pltpu.make_async_remote_copy(
            src_ref=counts.at[to, ys[2]] if direct else (sums_to, counts_to)[k].at[d],
            dst_ref=(sums_chip, counts_chip)[k].at[i],
            send_sem=chip_send.at[4 * k + i],
            recv_sem=chip_recv.at[4 * k + i],
            device_id={"member": 2 * ys[d] + to},
            device_id_type=MESH,
        )

    chip_copies = [(1, 1, 0), (1, 3, 0), (0, 1, 0), (0, 3, 0), (1, 2, 0), (1, 2, 1), (0, 2, 0)]
    core_copies = [(1, 1), (1, 3), (0, 2), (0, 1), (0, 3), (1, 0), (0, 0)]

    for turn in range(2):
        chip_copy(1, 2, turn).start()
    for copy in core_copies:
        if copy[0]:
            core_copy(*copy).start()
    for peer in (*along_x, *along_z[3:5]):
        pl.semaphore_signal(line_sem, inc=1, device_id={"region": peer}, device_id_type=MESH)
    point_sums(ens_v, sums, EARLY, 16)
    for copy in core_copies:
        if not copy[0]:
            core_copy(*copy).start()
    for k, d in core_copies:
        own, came, total = ((sums, sums_core, sums_to), (counts, counts_core, counts_to))[k]
        core_copy(k, d).wait_recv()
        total[d] = own[core, ys[d]] + came[d]
        if d:
            chip_copy(k, d).start()
    pl.semaphore_wait(line_sem, len(along_x) + 2)
    for peer in along_z:
        pl.semaphore_signal(all_sem, inc=1, device_id={"region": peer}, device_id_type=MESH)

    sub = lax.broadcasted_iota(I32, (OWN, LANES), 0)
    lane = lax.broadcasted_iota(I32, (OWN, LANES), 1)
    ids_col = jnp.sum(
        jnp.where(lane == 2 * (OWN * y + sub) + core, own_v[...].astype(F32), 0.0),
        axis=1,
        keepdims=True,
    ).astype(I32)
    prior_mean, prior_var = looked_up((mean_v, ivar_v), ids_col)
    in_block = lane == (ids_col & 127)

    for copy in chip_copies:
        chip_copy(*copy).wait_recv()

    def summed(total, came, k, size=OWN):
        at = slice(k * OWN, k * OWN + size)
        terms = [came[i, at, :] for i in range(came.shape[0])]
        return total[0, at, :] + sum(terms[1:], terms[0])

    mean = summed(sums_to, sums_chip, 0) * (1.0 / 80.0)
    first = core * HALF + y * OWN
    my_rows = pl.ds(pl.multiple_of(first, OWN), OWN)
    means[my_rows, :] = mean
    spread = (summed(sums_to, sums_chip, 1) - 80.0 * mean * mean) * (1.0 / 79.0)
    count, value, error = (summed(counts_to, counts_chip, k) for k in range(3))
    squares = summed(counts_to, counts_chip, 3, 2)
    mine = lane == sub + first

    def per_slot(x):
        return jnp.sum(x, axis=1, keepdims=True)

    innov_sum = per_slot(
        jnp.where(mine, squares[0:1], 0.0)
        + mean * (count * mean - 2.0 * value)
    )
    error_error = per_slot(jnp.where(mine, squares[1:2], 0.0))
    count_spread = count * spread
    spread_sum = per_slot(count_spread)
    spread_spread = per_slot(count_spread * spread)
    spread_error = per_slot(spread * error)
    error_sum = per_slot(error)
    weight_var = (
        2.0 * prior_mean * prior_mean * (1.0 + spread_spread)
        + 4.0 * prior_mean * spread_error
        + 2.0 * error_error
    )
    lam = jnp.maximum(
        (prior_mean * weight_var + prior_var * spread_sum * (innov_sum - error_sum))
        / (weight_var + prior_var * spread_sum * spread_sum),
        1.0,
    )
    placed = jnp.where(in_block, lam, 0.0)
    for r in range(32):
        to_region[r] = jnp.sum(
            jnp.where((ids_col >> 7) == r, placed, 0.0), axis=0, keepdims=True
        )
    my_lam[...] = jnp.sum(jnp.where(mine, lam, 0.0), axis=0, keepdims=True)

    def to_all(some):
        for i, (peer, dest) in some:
            pltpu.make_async_remote_copy(
                src_ref=to_region.at[peer],
                dst_ref=from_region.at[pl.ds(i, 1)],
                send_sem=reg_send,
                recv_sem=reg_recv,
                device_id={"region": peer, "member": dest},
                device_id_type=MESH,
            ).start()

    everyone = list(enumerate(peers))
    pl.semaphore_wait(all_sem, len(along_z))
    to_all(everyone[:96])
    lam_copies = []
    for i, peer in enumerate(others):
        lam_copies.append(
            pltpu.make_async_remote_copy(
                src_ref=my_lam,
                dst_ref=lams.at[i],
                send_sem=lam_send.at[i],
                recv_sem=lam_recv.at[i],
                device_id={"member": peer},
                device_id_type=MESH,
            )
        )
        lam_copies[-1].start()
    mean_copies = []
    for i, peer in enumerate(others):
        mean_copies.append(
            pltpu.make_async_remote_copy(
                src_ref=means.at[my_rows],
                dst_ref=means.at[my_rows],
                send_sem=mean_send.at[i],
                recv_sem=mean_recv.at[i],
                device_id={"member": peer},
                device_id_type=MESH,
            )
        )
        mean_copies[-1].start()

    to_all(everyone[96:])
    for copy in lam_copies:
        copy.wait_recv()
    lam_row = my_lam[...]
    for i in range(len(others)):
        lam_row = lam_row + lams[i]
    eye = lax.broadcasted_iota(I32, (LANES, LANES), 0) == lax.broadcasted_iota(
        I32, (LANES, LANES), 1
    )
    lam_col = jnp.sum(jnp.where(eye, lam_row, 0.0), axis=1, keepdims=True)
    scale[...] = jnp.broadcast_to(jnp.sqrt(lam_col), (LANES, LANES))
    for copy in mean_copies:
        copy.wait_recv()

    @pl.loop(0, 16)
    def _(j):
        for i in range(8):
            at = pl.ds(pl.multiple_of(j * 1024 + i * LANES, LANES), LANES)
            row = pl.ds(HALF * (i % 2) + 4 * j + i // 2, 1)
            m = means[row, :]
            x = ens_v[:, at].astype(F32)
            out[:, at] = (m + scale[row, :] * (x - m)).astype(BF16)

    arrived = pltpu.make_async_remote_copy(
        src_ref=from_region.at[0:255],
        dst_ref=from_region.at[0:255],
        send_sem=reg_send,
        recv_sem=reg_recv,
        device_id={"member": others[0]},
        device_id_type=MESH,
    )
    for copy in core_copies:
        core_copy(*copy).wait_send()
    for copy in chip_copies:
        chip_copy(*copy).wait_send()
    for copy in (*mean_copies, *lam_copies, arrived):
        copy.wait_send()
    arrived.wait_recv()
    post_row = to_region[region] + jnp.sum(from_region[...], axis=0, keepdims=True)
    turned = pltpu.roll(jnp.broadcast_to(post_row, (8, LANES)), (8 - member) * OWN % LANES, 1)
    post[...] = turned[0:1, :OWN]


def written(a, b, a_out, b_out, sem):
    copies = [
        pltpu.make_async_copy(a, a_out, sem.at[0]),
        pltpu.make_async_copy(b, b_out, sem.at[1]),
    ]
    for copy in copies:
        copy.start()
    for copy in copies:
        copy.wait()


def body(ensemble, obs_value, obs_var, obs_point, owned_blocks, infl_mean, infl_var):
    anywhere = pl.BlockSpec(memory_space=pl.ANY)
    vmem = pl.BlockSpec(memory_space=pltpu.VMEM)
    dma = pltpu.SemaphoreType.DMA
    inflated, post = pl.pallas_call(
        kernel,
        out_shape=(pltpu.VMEM(ensemble.shape, BF16), pltpu.VMEM((1, OWN), F32)),
        in_specs=[anywhere] * 7,
        out_specs=(vmem, vmem),
        scratch_shapes=[
            pltpu.VMEM((10, 16384), BF16),
            pltpu.VMEM((32, LANES), F32),
            pltpu.VMEM((32, LANES), F32),
            pltpu.VMEM((32, LANES), I32),
            pltpu.VMEM((1, LANES), I32),
            pltpu.VMEM((32, LANES), F32),
            pltpu.VMEM((32, LANES), F32),
            pltpu.VMEM((14, 32, LANES), F32),
            pltpu.VMEM((5 * HALF, 2 * LANES), F32),
            pltpu.VMEM((8, HALF), F32),
            *[
                pltpu.VMEM((*lead, rows, LANES), F32)
                for lead in ((2, 4), (4,), (4,))
                for rows in (POINTS, COUNTS)
            ],
            pltpu.VMEM((3, POINTS, LANES), F32),
            pltpu.VMEM((4, COUNTS, LANES), F32),
            pltpu.VMEM((LANES, LANES), F32),
            pltpu.VMEM((1, LANES), F32),
            pltpu.VMEM((7, 1, LANES), F32),
            pltpu.VMEM((LANES, LANES), F32),
            pltpu.VMEM((32, 1, LANES), F32),
            pltpu.VMEM((256, LANES), F32),
            dma((7,)),
            pltpu.SemaphoreType.REGULAR,
            pltpu.SemaphoreType.REGULAR,
            *[dma((n,)) for n in (8, 8, 7, 7) for _ in range(2)],
            dma,
            dma,
        ],
        compiler_params=pltpu.CompilerParams(collective_id=0, has_side_effects=True),
    )(
        ensemble,
        obs_value,
        obs_var,
        obs_point,
        owned_blocks.reshape(1, -1),
        infl_mean.reshape(32, LANES),
        infl_var.reshape(32, LANES),
    )
    inflated, post = pl.pallas_call(
        written,
        out_shape=(
            jax.ShapeDtypeStruct(ensemble.shape, BF16),
            jax.ShapeDtypeStruct((1, OWN), F32),
        ),
        in_specs=(vmem, vmem),
        out_specs=(anywhere, anywhere),
        scratch_shapes=[dma((2,))],
    )(
        pltpu.with_memory_space_constraint(inflated, pltpu.VMEM),
        pltpu.with_memory_space_constraint(post, pltpu.VMEM),
    )
    return inflated, post.reshape(-1)


def solution(mesh):
    placed = (
        P("member", "region"),
        P(("region", "member"), None),
        P(("region", "member"), None),
        P(("region", "member"), None),
        P("region"),
        P(),
        P(),
    )
    return jax.shard_map(
        body,
        mesh=mesh,
        in_specs=placed,
        out_specs=(P("member", "region"), P(("region", "member"))),
        check_vma=False,
    )
```
